128 devices in a mesh: rep: 2 (over core), dp: 64 (over x, y, z).
Axes of the slice: x: 4, y: 4, z: 4, core: 2. Of those that a mesh axis runs over, the one named last changes fastest.
Arguments:
- x: bfloat16 [128, 2048, 1024], P(('rep', 'dp')), parts along dimension 0
- dy: bfloat16 [128, 2048, 1024], P(('rep', 'dp')), parts along dimension 0
- w_gate: bfloat16 [2, 1024, 3328], replicated
- w_up: bfloat16 [2, 1024, 3328], replicated
- w_down: bfloat16 [2, 3328, 1024], replicated
- m_w_gate: float32 [2, 1024, 3328], replicated
- m_w_up: float32 [2, 1024, 3328], replicated
- m_w_down: float32 [2, 3328, 1024], replicated
- v_w_gate: float32 [2, 1024, 3328], replicated
- v_w_up: float32 [2, 1024, 3328], replicated
- v_w_down: float32 [2, 3328, 1024], replicated
Outputs:
- output 1: bfloat16 [4, 1024, 3328], P('rep'), parts along dimension 0
- output 2: bfloat16 [4, 1024, 3328], P('rep'), parts along dimension 0
- output 3: bfloat16 [4, 3328, 1024], P('rep'), parts along dimension 0
- output 4: float32 [4, 1024, 3328], P('rep'), parts along dimension 0
- output 5: float32 [4, 1024, 3328], P('rep'), parts along dimension 0
- output 6: float32 [4, 3328, 1024], P('rep'), parts along dimension 0
- output 7: float32 [4, 1024, 3328], P('rep'), parts along dimension 0
- output 8: float32 [4, 1024, 3328], P('rep'), parts along dimension 0
- output 9: float32 [4, 3328, 1024], P('rep'), parts along dimension 0
There are 2 independent parts. The reference program is written for one: setup_inputs(seed, part) draws one part's arguments, and reference() takes and returns one part's arrays. A program takes and returns all parts, laid end to end along the dimension named above; an argument that names none is the same for every part.
All inputs are finite; a program needn't handle non-finite values.
Results may differ from the reference program's by a relative error of at most 0.022.
Values are sent between devices in bfloat16 or wider.
A program may use at most 1.5 GiB of HBM per device.

```python
import jax
import jax.numpy as jnp
from jax import lax

SEQUENCES = 64
TOKENS = 2048
D = 1024
FF = 3328
LAYERS = 2
NAMES = ("w_gate", "w_up", "w_down")
SHAPES = {"w_gate": (LAYERS, D, FF), "w_up": (LAYERS, D, FF), "w_down": (LAYERS, FF, D)}


def bump(key, n, height):
    away = (jnp.arange(n, dtype=jnp.int32) - jax.random.randint(key, (), 0, n, jnp.int32)) % n
    return jnp.where(away < n // 8, height, 1.0)


def together(key, own, strength):
    shared = jax.random.normal(key, own.shape[1:], jnp.float32)
    return (own + strength * shared) * lax.rsqrt(1 + strength * strength)


def setup_inputs(seed: int = 0, part: int = 0) -> dict:
    kx, kdy, ka, kb, kz, kf, kh, kl, *keys = jax.random.split(jax.random.key(seed), 8 + 3 * len(NAMES))
    kx, kdy, ka, kb = (jax.random.fold_in(k, part) for k in (kx, kdy, ka, kb))
    kw, km, kv = (keys[i::3] for i in range(3))
    shape = (SEQUENCES, TOKENS, D)
    much_x, much_dy = jax.random.uniform(kz, (2,), jnp.float32, 0.0, 1.0)
    loud = 2.0 ** jax.random.uniform(jax.random.fold_in(kz, 1), (), jnp.float32, -1.0, 2.0)
    layers = 2.0 ** jax.random.uniform(kl, (LAYERS, 1, 1), jnp.float32, -1.0, 1.0)
    x = together(ka, jax.random.normal(kx, shape, jnp.float32), much_x) * bump(kf, D, 4.0)
    dy = together(kb, jax.random.normal(kdy, shape, jnp.float32), much_dy)
    drawn = {"x": x.astype(jnp.bfloat16), "dy": (loud * dy * (SEQUENCES * TOKENS) ** -0.5).astype(jnp.bfloat16)}
    for key, name in zip(kw, NAMES, strict=True):
        w = jax.random.normal(key, SHAPES[name], jnp.float32) * SHAPES[name][1] ** -0.5
        drawn[name] = (w * {"w_gate": 1.0, "w_up": bump(kh, FF, 4.0), "w_down": layers}[name]).astype(jnp.bfloat16)
    for key, name in zip(km, NAMES, strict=True):
        drawn[f"m_{name}"] = 0.1 * jax.random.normal(key, SHAPES[name], jnp.float32)
    for key, name in zip(kv, NAMES, strict=True):
        drawn[f"v_{name}"] = loud * loud * jax.random.uniform(key, SHAPES[name], jnp.float32, 0.05, 0.15)
    return drawn


def matmul(a, w):
    return jnp.dot(a, w, preferred_element_type=jnp.float32).astype(jnp.bfloat16)


def normed(h):
    wide = h.astype(jnp.float32)
    scale = lax.rsqrt(jnp.mean(wide**2, -1, keepdims=True) + 1e-6)
    return (wide * scale).astype(jnp.bfloat16)


def layer(h, w):
    a = normed(h)
    gate = jnp.dot(a, w["w_gate"], preferred_element_type=jnp.float32)
    up = jnp.dot(a, w["w_up"], preferred_element_type=jnp.float32)
    return h + matmul((jax.nn.silu(gate) * up).astype(jnp.bfloat16), w["w_down"])


def adamw(w, m, v, g):
    m = 0.9 * m + 0.1 * g
    v = 0.95 * v + 0.05 * g * g
    step = m * lax.rsqrt(v + 1e-8) + 0.1 * w
    return (w - 0.02 * step).astype(jnp.bfloat16), m, v


def stack(weights, h):
    return lax.scan(lambda h, w: (layer(h, w), None), h, weights)[0]


def reference(x, dy, w_gate, w_up, w_down, m_w_gate, m_w_up, m_w_down, v_w_gate, v_w_up, v_w_down):
    weights = dict(zip(NAMES, (w_gate, w_up, w_down), strict=True))

    def take(so_far, sequence):
        h, by_y = sequence
        _, back = jax.vjp(lambda w: stack(w, h), weights)
        return jax.tree.map(lambda total, term: total + term.astype(jnp.float32), so_far, back(by_y)[0]), None

    none_yet = {name: jnp.zeros(w.shape, jnp.float32) for name, w in weights.items()}
    by_weights, _ = lax.scan(take, none_yet, (x, dy))
    gradients = [by_weights[name].astype(jnp.bfloat16).astype(jnp.float32) for name in NAMES]
    new = [
        adamw(w.astype(jnp.float32), m, v, g)
        for w, m, v, g in zip((w_gate, w_up, w_down), (m_w_gate, m_w_up, m_w_down), (v_w_gate, v_w_up, v_w_down), gradients, strict=True)
    ]
    return tuple(one[which] for which in range(3) for one in new)
```

```python
import functools

import jax
import jax.numpy as jnp
from jax import lax
from jax.experimental import pallas as pl
from jax.experimental.pallas import tpu as pltpu
from jax.sharding import PartitionSpec as P

T, D, FF, SL = 2048, 1024, 3328, 256
NS = FF // SL
TB = 512
F32, BF = jnp.float32, jnp.bfloat16
MESH = pl.DeviceIdType.MESH
VMEM_LIMIT = 66_900_000
COMM = True

OFF = (0, 2, 5, 7, 9, 11, 13, 15, 17, 19, 21, 24, 26)
NR = 12
SLOTS = 3


def dot(a, b):
    return lax.dot_general(a, b, (((1,), (0,)), ((), ())), preferred_element_type=F32)


def dot_nt(a, b):
    return lax.dot_general(a, b, (((1,), (1,)), ((), ())), preferred_element_type=F32)


def normed(h):
    wide = h.astype(F32)
    scale = lax.rsqrt(jnp.mean(wide * wide, -1, keepdims=True) + 1e-6)
    return (wide * scale).astype(BF)


def forward_kernel(x_ref, dy_ref, wg_ref, wu_ref, wd_ref, gate_ref, up_ref, h1_ref, a1_ref, a0t_ref, a1t_ref, dyt_ref, a0, acc, stage, sem):
    j = pl.program_id(0)

    @pl.when(j == 0)
    def _():
        def one(b, c):
            rows = pl.ds(pl.multiple_of(b * TB, TB), TB)
            a = normed(x_ref[rows, :])
            a0[rows, :] = a
            acc[rows, :] = jnp.zeros((TB, D), F32)
            return c

        lax.fori_loop(0, T // TB, one, 0)

    def transposed(src, dst):
        def one(b, c):
            rows = pl.ds(pl.multiple_of(b * TB, TB), TB)
            stage[:, rows] = src[rows, :].T
            return c

        lax.fori_loop(0, T // TB, one, 0)
        copy = pltpu.make_async_copy(stage, dst, sem)
        copy.start()
        copy.wait()

    @pl.when(j == 1)
    def _():
        transposed(a0, a0t_ref)

    @pl.when(j == 2)
    def _():
        transposed(dy_ref, dyt_ref)

    def one(b, c):
        rows = pl.ds(pl.multiple_of(b * TB, TB), TB)
        a = a0[rows, :]
        gate = dot(a, wg_ref[0])
        up = dot(a, wu_ref[0])
        gate_ref[0, rows, :] = gate
        up_ref[0, rows, :] = up
        hid = (gate * jax.nn.sigmoid(gate) * up).astype(BF)
        acc[rows, :] += dot(hid, wd_ref[0])
        return c

    lax.fori_loop(0, T // TB, one, 0)

    @pl.when(j == NS - 1)
    def _():
        def one(b, c):
            rows = pl.ds(pl.multiple_of(b * TB, TB), TB)
            h1 = (x_ref[rows, :].astype(F32) + acc[rows, :].astype(BF).astype(F32)).astype(BF)
            h1_ref[rows, :] = h1
            a1_ref[rows, :] = normed(h1)
            return c

        lax.fori_loop(0, T // TB, one, 0)
        transposed(a1_ref, a1t_ref)


def forward(x, dy, wg, wu, wd):
    whole = pl.BlockSpec((T, D), lambda j: (0, 0))
    wide = pl.BlockSpec((1, T, SL), lambda j: (j, 0, 0))
    anyspec = pl.BlockSpec(memory_space=pl.ANY)
    return pl.pallas_call(
        forward_kernel,
        name="forward",
        grid=(NS,),
        in_specs=[
            whole,
            whole,
            pl.BlockSpec((1, D, SL), lambda j: (0, 0, j)),
            pl.BlockSpec((1, D, SL), lambda j: (0, 0, j)),
            pl.BlockSpec((1, SL, D), lambda j: (0, j, 0)),
        ],
        out_specs=[wide, wide, whole, whole, anyspec, anyspec, anyspec],
        out_shape=[
            jax.ShapeDtypeStruct((NS, T, SL), F32),
            jax.ShapeDtypeStruct((NS, T, SL), F32),
            jax.ShapeDtypeStruct((T, D), BF),
            jax.ShapeDtypeStruct((T, D), BF),
            jax.ShapeDtypeStruct((D, T), BF),
            jax.ShapeDtypeStruct((D, T), BF),
            jax.ShapeDtypeStruct((D, T), BF),
        ],
        scratch_shapes=[pltpu.VMEM((T, D), BF), pltpu.VMEM((T, D), F32), pltpu.VMEM((D, T), BF), pltpu.SemaphoreType.DMA],
        compiler_params=pltpu.CompilerParams(vmem_limit_bytes=VMEM_LIMIT),
        cost_estimate=pl.CostEstimate(flops=6 * T * D * FF, bytes_accessed=100_000_000, transcendentals=T * FF),
    )(x, dy, wg, wu, wd)


def backward_kernel(
    a1_ref, dy_ref, a1t_ref, dyt_ref, h1_ref, a0t_ref, gate_ref, up_ref, wg_ref, wu_ref, wd_ref,
    g1_ref, g0_ref,
    act, by, actt, byt, acc, hid, dgt, dup, wgb, wub, wdb,
    grad, s1, s2, sa0, ra0, sb0, rb0, sa1, ra1, sb1, rb1, sa2, ra2, sb2, rb2, cb, g0b,
    wsem, asem, lsem, send, recv,
):
    me = lax.axis_index("dp")
    xyz = (lax.div(me, 16), lax.rem(lax.div(me, 4), 4), lax.rem(me, 4))
    stride = (16, 4, 1)
    axes = [[(m + k) % 3 for k in range(3)] for m in range(3)]
    plus = [me + (lax.rem(xyz[d] + 1, 4) - xyz[d]) * stride[d] for d in range(3)]
    minus = [me + (lax.rem(xyz[d] + 3, 4) - xyz[d]) * stride[d] for d in range(3)]
    digit = [[xyz[d] for d in axes[m]] for m in range(3)]
    to = [[(plus[d], minus[d]) for d in axes[m]] for m in range(3)]

    def turn(c, k):
        return lax.rem(c + k, 4)

    def block(c, size):
        return pl.ds(pl.multiple_of(c * size, size), size)

    if COMM:
        barrier = pltpu.get_barrier_semaphore()
        for d in range(3):
            for n in (plus[d], minus[d]):
                pl.semaphore_signal(barrier, inc=1, device_id={"dp": n}, device_id_type=MESH)
        pl.semaphore_wait(barrier, 6)

    HALF = (pl.ds(0, 128), pl.ds(128, 128))
    sas, ras, sbs, rbs = (sa0, sa1, sa2), (ra0, ra1, ra2), (sb0, sb1, sb2), (rb0, rb1, rb2)
    sizes = (256, 64, 16)

    def parts(r, s, m, k):
        two, three = lax.rem(s, 2), lax.rem(s, 3)
        if r < 6:
            ph = r // 2
            if r % 2 == 0:
                return sas[ph].at[two, m, k], ras[ph].at[two, m, k]
            slot = three if ph == 0 else two
            return sbs[ph].at[slot, m, k], rbs[ph].at[slot, m, k]
        eight = lax.rem(s, 8)
        ph = 2 - (r - 6) // 2
        c = digit[m][ph]
        size = sizes[ph]
        if ph == 0:
            if r % 2 == 0:
                return cb.at[eight, m], g1_ref.at[m, s, block(c, size)]
            ref = g1_ref.at[m, s, block(turn(c, 3 if k == 0 else 1), size), HALF[k]]
            return ref, ref
        base = block(digit[m][1] * 4 + c, size) if ph == 2 else block(c, size)
        if r % 2 == 0:
            return cb.at[eight, m, base], cb.at[eight, m, base]
        c = turn(c, 3 if k == 0 else 1)
        base = block(digit[m][1] * 4 + c, size) if ph == 2 else block(c, size)
        return cb.at[eight, m, base, HALF[k]], cb.at[eight, m, base, HALF[k]]

    def copies(r, s):
        slot = lax.rem(s, SLOTS)
        ph = r // 2 if r < 6 else 2 - (r - 6) // 2
        for m in range(3):
            for k in range(2):
                src, dst = parts(r, s, m, k)
                yield pltpu.make_async_remote_copy(
                    src_ref=src,
                    dst_ref=dst,
                    send_sem=send.at[r, slot, m, k],
                    recv_sem=recv.at[r, slot, m, k],
                    device_id={"dp": to[m][ph][k]},
                    device_id_type=MESH,
                )

    def finish(r, s):
        for copy in copies(r, s):
            copy.wait()

    def own_copy(s, m):
        return pltpu.make_async_copy(
            cb.at[lax.rem(s, 8), m], g1_ref.at[m, s, block(digit[m][0], 256)], lsem.at[lax.rem(s, SLOTS), m]
        )

    def prepare(r, s):
        two, three, eight = lax.rem(s, 2), lax.rem(s, 3), lax.rem(s, 8)
        if r > 0:
            finish(r - 1, s)
        if r <= 6:
            ph = r // 2
            size = sizes[min(ph, 2)]
            total = (grad, s1, s2)[min(ph, 2)]
            for m in range(3):
                if r % 2 == 0 and r > 0:
                    before = (grad, s1, s2)[ph - 1]
                    slot = three if ph == 1 else two
                    mine = before[three, m, block(digit[m][ph - 1], sizes[ph - 1]), :]
                    mine = mine + rbs[ph - 1][slot, m, 0].astype(F32) + rbs[ph - 1][slot, m, 1].astype(F32)
                    if r < 6:
                        total[three, m] = mine
                    else:
                        done = mine.astype(BF)

                        @pl.when(s < NS)
                        def _():
                            cb[eight, m, block(digit[m][1] * 4 + digit[m][2], 16), :] = done

                        @pl.when(s >= NS)
                        def _():
                            g0b[m, s - NS] = done

                if r < 6 and r % 2 == 0:
                    far = block(turn(digit[m][ph], 2), size)
                    for k in range(2):
                        sas[ph][two, m, k] = total[three, m, far, HALF[k]].astype(BF)
                if r < 6 and r % 2 == 1:
                    slot = three if ph == 0 else two
                    for k in range(2):
                        near = block(turn(digit[m][ph], 1 if k == 0 else 3), size)
                        add, keep = HALF[k], HALF[1 - k]
                        sbs[ph][slot, m, k, :, add] = (total[three, m, near, add] + ras[ph][two, m, k].astype(F32)).astype(BF)
                        sbs[ph][slot, m, k, :, keep] = total[three, m, near, keep].astype(BF)
        if r == NR:
            for m in range(3):
                own_copy(s, m).wait()

    def start(r, s):
        for copy in copies(r, s):
            copy.start()
        if r == 10:
            for m in range(3):
                own_copy(s, m).start()

    def service(i, half):
        if not COMM:
            return
        todo = []
        for r in range(NR + 1):
            if OFF[r] % 2 == (1 - half):
                back = (OFF[r] + 1 - half) // 2
                todo.append((r, back))
        for r, back in todo:
            s = i - back

            @pl.when((s >= 0) & (s < (2 * NS if r <= 6 else NS)))
            def _():
                prepare(r, s)

        for r, back in todo:
            if r == NR:
                continue
            s = i - back

            @pl.when((s >= 0) & (s < (2 * NS if r < 6 else NS)))
            def _():
                start(r, s)

    def weights(i):
        slot = lax.rem(i, 2)
        first = i < NS
        j = lax.rem(i, NS)
        columns = block(j, SL)
        down = pltpu.make_async_copy(wd_ref.at[jnp.where(first, 1, 0), columns, :], wdb.at[slot], wsem.at[slot, 0])
        one = [
            pltpu.make_async_copy(wg_ref.at[1, :, columns], wgb.at[slot], wsem.at[slot, 1]),
            pltpu.make_async_copy(wu_ref.at[1, :, columns], wub.at[slot], wsem.at[slot, 2]),
        ]
        zero = [
            pltpu.make_async_copy(gate_ref.at[j], acc.at[2 * slot], wsem.at[slot, 1]),
            pltpu.make_async_copy(up_ref.at[j], acc.at[2 * slot + 1], wsem.at[slot, 2]),
        ]
        return down, one, zero

    loads = [
        pltpu.make_async_copy(a1_ref, act, asem.at[0]),
        pltpu.make_async_copy(dy_ref, by, asem.at[1]),
        pltpu.make_async_copy(a1t_ref, actt, asem.at[2]),
        pltpu.make_async_copy(dyt_ref, byt, asem.at[3]),
    ]
    down, one, _ = weights(0)
    for copy in [down, *one, *loads]:
        copy.start()

    def clear(b, c):
        rows = block(b, TB)
        for n in range(4):
            acc[n, rows, :] = jnp.zeros((TB, SL), F32)
        return c

    lax.fori_loop(0, T // TB, clear, 0)
    loads[0].wait()
    loads[1].wait()
    h1_load = pltpu.make_async_copy(h1_ref, act, asem.at[0])
    a0t_load = pltpu.make_async_copy(a0t_ref, actt, asem.at[2])

    def second_layer(i):
        slot = lax.rem(i, 2)
        down, one, _ = weights(i)
        for copy in [down, *one]:
            copy.wait()

        @pl.when(i + 1 < NS)
        def _():
            down, one, _ = weights(i + 1)
            for copy in [down, *one]:
                copy.start()

        def tokens(b, c):
            rows = block(b, TB)
            a = act[rows, :]
            gate = dot(a, wgb[slot])
            up = dot(a, wub[slot])
            by_hid = dot_nt(by[rows, :], wdb[slot]).astype(BF).astype(F32)
            sig = jax.nn.sigmoid(gate)
            silu = gate * sig
            hid[rows, :] = (silu * up).astype(BF)
            by_up = (by_hid * silu).astype(BF)
            by_gate = (by_hid * up * (sig * (1.0 + gate * (1.0 - sig)))).astype(BF)
            dup[rows, :] = by_up
            dgt[rows, :] = by_gate
            for n in range(4):
                acc[n, rows, :] += dot_nt(by_gate, wgb[slot, pl.ds(n * SL, SL), :]) + dot_nt(by_up, wub[slot, pl.ds(n * SL, SL), :])
            return c

        lax.fori_loop(0, T // TB, tokens, 0)

    def between(i):
        h1_load.wait()
        a0t_load.start()
        down, _, zero = weights(i)
        down.start()

        def tokens(b, c):
            rows = pl.ds(pl.multiple_of(b * 256, 256), 256)
            wide = act[rows, :].astype(F32)
            scale = lax.rsqrt(jnp.mean(wide * wide, -1, keepdims=True) + 1e-6)
            da = jnp.concatenate([acc[n, rows, :] for n in range(4)], axis=1).astype(BF).astype(F32)
            t = jnp.mean(da * wide, -1, keepdims=True)
            dwide = (da * scale - wide * (scale * scale * scale * t)).astype(BF)
            by_h = (by[rows, :].astype(F32) + dwide.astype(F32)).astype(BF)
            by[rows, :] = by_h
            byt[:, rows] = by_h.T
            return c

        lax.fori_loop(0, T // 256, tokens, 0)
        for copy in zero:
            copy.start()
        a0t_load.wait()

    def first_layer(i):
        slot = lax.rem(i, 2)

        @pl.when(i == NS)
        def _():
            between(i)

        down, _, zero = weights(i)
        for copy in [down, *zero]:
            copy.wait()

        @pl.when(i + 1 < 2 * NS)
        def _():
            down, _, zero = weights(i + 1)
            for copy in [down, *zero]:
                copy.start()

        def tokens(b, c):
            rows = block(b, TB)
            gate = acc[2 * slot, rows, :]
            up = acc[2 * slot + 1, rows, :]
            by_hid = dot_nt(by[rows, :], wdb[slot]).astype(BF).astype(F32)
            sig = jax.nn.sigmoid(gate)
            silu = gate * sig
            hid[rows, :] = (silu * up).astype(BF)
            dup[rows, :] = (by_hid * silu).astype(BF)
            dgt[rows, :] = (by_hid * up * (sig * (1.0 + gate * (1.0 - sig)))).astype(BF)
            return c

        lax.fori_loop(0, T // TB, tokens, 0)

    def iteration(i, c):
        @pl.when(i < NS)
        def _():
            second_layer(i)

        @pl.when(i == 0)
        def _():
            loads[2].wait()
            loads[3].wait()

        @pl.when(i == NS - 1)
        def _():
            h1_load.start()

        @pl.when((i >= NS) & (i < 2 * NS))
        def _():
            first_layer(i)

        service(i, 0)

        @pl.when(i < 2 * NS)
        def _():
            three = lax.rem(i, 3)
            for m, (left, right) in enumerate(((actt, dgt), (actt, dup), (byt, hid))):
                grad[three, m] = dot(left[...], right[...])

        service(i, 1)
        return c

    count = max(2 * NS + 7, NS + 14) if COMM else 2 * NS
    lax.fori_loop(0, count, iteration, 0)
    out = pltpu.make_async_copy(g0b, g0_ref, asem.at[0])
    out.start()
    out.wait()


def backward(a1, dy, a1t, dyt, h1, a0t, gate, up, wg, wu, wd):
    anyspec = pl.BlockSpec(memory_space=pl.ANY)
    V = pltpu.VMEM
    DMA = pltpu.SemaphoreType.DMA
    return pl.pallas_call(
        backward_kernel,
        name="backward",
        in_specs=[anyspec] * 11,
        out_specs=[anyspec] * 2,
        out_shape=[jax.ShapeDtypeStruct((3, NS, D, SL), BF), jax.ShapeDtypeStruct((3, NS, 16, SL), BF)],
        scratch_shapes=[
            V((T, D), BF), V((T, D), BF), V((D, T), BF), V((D, T), BF), V((4, T, SL), F32),
            V((T, SL), BF), V((T, SL), BF), V((T, SL), BF),
            V((2, D, SL), BF), V((2, D, SL), BF), V((2, SL, D), BF),
            V((3, 3, 1024, SL), F32), V((3, 3, 256, SL), F32), V((3, 3, 64, SL), F32),
            V((2, 3, 2, 256, 128), BF), V((2, 3, 2, 256, 128), BF), V((3, 3, 2, 256, SL), BF), V((3, 3, 2, 256, SL), BF),
            V((2, 3, 2, 64, 128), BF), V((2, 3, 2, 64, 128), BF), V((2, 3, 2, 64, SL), BF), V((2, 3, 2, 64, SL), BF),
            V((2, 3, 2, 16, 128), BF), V((2, 3, 2, 16, 128), BF), V((2, 3, 2, 16, SL), BF), V((2, 3, 2, 16, SL), BF),
            V((8, 3, 256, SL), BF), V((3, NS, 16, SL), BF),
            DMA((2, 3)), DMA((4,)), DMA((SLOTS, 3)), DMA((NR, SLOTS, 3, 2)), DMA((NR, SLOTS, 3, 2)),
        ],
        compiler_params=pltpu.CompilerParams(vmem_limit_bytes=VMEM_LIMIT, collective_id=0 if COMM else None, has_side_effects=True),
        cost_estimate=pl.CostEstimate(flops=24 * T * D * FF, bytes_accessed=150_000_000, transcendentals=2 * T * FF),
    )(a1, dy, a1t, dyt, h1, a0t, gate, up, wg, wu, wd)


def adam_kernel(gathered, *refs):
    ins, rest = refs[:12], refs[12:]
    if gathered:
        rest = rest[9:]
    outs, rest = rest[:9], rest[9:]
    for m in range(3):
        w_ref, m_ref, v_ref, g_ref = ins[m], ins[3 + m], ins[6 + m], ins[9 + m]
        w_out, m_out, v_out = outs[m], outs[3 + m], outs[6 + m]

        def take(at, g):
            g = g.astype(F32)
            w = w_ref[at].astype(F32)
            mean = 0.9 * m_ref[at] + 0.1 * g
            var = 0.95 * v_ref[at] + 0.05 * g * g
            w_out[at] = (w - 0.02 * (mean * lax.rsqrt(var + 1e-8) + 0.1 * w)).astype(BF)
            m_out[at] = mean
            v_out[at] = var

        if gathered:
            whole = rest[0]
            for n in range(64):
                digits = (n // 16, n // 4 % 4, n % 4)
                xyz = [digits[(d - m) % 3] for d in range(3)]
                whole[n * 16 : n * 16 + 16, :] = g_ref[xyz[0] * 16 + xyz[1] * 4 + xyz[2], 0, 0]
            look = lambda rows: whole[rows, :]
        else:
            look = lambda rows: g_ref[0, 0, rows, :]

        if m < 2:

            def one(b, c):
                rows = pl.ds(pl.multiple_of(b * 64, 64), 64)
                take((0, rows, slice(None)), look(rows))
                return c

            lax.fori_loop(0, D // 64, one, 0)
        else:

            def one(b, c):
                rows = pl.ds(pl.multiple_of(b * 128, 128), 128)
                take((0, slice(None), rows), look(rows).T)
                return c

            lax.fori_loop(0, D // 128, one, 0)


def adam(layer, weights, means, variances, gradients, so_far=None):
    wide = pl.BlockSpec((1, D, SL), lambda j: (layer, 0, j))
    tall = pl.BlockSpec((1, SL, D), lambda j: (layer, j, 0))
    mine = [wide, wide, tall]
    gathered = so_far is not None
    if gathered:
        grads = [pl.BlockSpec((64, 1, 1, 16, SL), functools.partial(lambda m, j: (0, m, j, 0, 0), m)) for m in range(3)]
    else:
        grads = [pl.BlockSpec((1, 1, D, SL), functools.partial(lambda m, j: (m, j, 0, 0), m)) for m in range(3)]
    shapes = [jax.ShapeDtypeStruct(a.shape, a.dtype) for a in (*weights, *means, *variances)]
    return pl.pallas_call(
        functools.partial(adam_kernel, gathered),
        name=f"adam{layer}",
        grid=(NS,),
        in_specs=mine * 3 + grads + ([pl.BlockSpec(memory_space=pl.ANY)] * 9 if gathered else []),
        out_specs=mine * 3,
        out_shape=shapes,
        input_output_aliases={12 + k: k for k in range(9)} if gathered else {},
        scratch_shapes=[pltpu.VMEM((D, SL), BF)] if gathered else [],
        compiler_params=pltpu.CompilerParams(vmem_limit_bytes=VMEM_LIMIT),
        cost_estimate=pl.CostEstimate(flops=10**10, bytes_accessed=66 * D * FF, transcendentals=3 * D * FF),
    )(*weights, *means, *variances, *[gradients] * 3, *(so_far or ()))


def solution(mesh):
    def step(x, dy, *arrays):
        x, dy = x[0], dy[0]
        weights, means, variances = (arrays[k : k + 3] for k in (0, 3, 6))
        gate, up, h1, a1, a0t, a1t, dyt = forward(x, dy, *weights)
        g1, g0 = backward(a1, dy, a1t, dyt, h1, a0t, gate, up, *weights)
        g0 = lax.all_gather(g0, "dp", axis=0)
        new = adam(1, weights, means, variances, g1)
        return tuple(adam(0, weights, means, variances, g0, new))

    return jax.shard_map(
        step,
        mesh=mesh,
        in_specs=(P(("rep", "dp"), None, None),) * 2 + (P(None, None, None),) * 9,
        out_specs=(P("rep", None, None),) * 9,
        check_vma=False,
    )
```

```python
import functools

import jax
import jax.numpy as jnp
from jax import lax
from jax.experimental import pallas as pl
from jax.experimental.pallas import tpu as pltpu
from jax.sharding import PartitionSpec as P

T, D, FF, SL = 2048, 1024, 3328, 256
NS = FF // SL
TB = 512
H = 256
FB, FH = 2048, 512
F32, BF = jnp.float32, jnp.bfloat16
MESH = pl.DeviceIdType.MESH
VMEM_LIMIT = 66_900_000

STEPS1, MID, STEPS0 = 4, 4, 2
START0 = STEPS1 * NS + MID
OFF = (0, 2, 5, 7, 9, 11, 13, 15, 17, 20, 23, 29, 32)
NR = 12
SLOTS, SEMS, GRADS, CB = 4, 4, 4, 8
Q = 3
CUT = 2


def dot(a, b):
    return lax.dot_general(a, b, (((1,), (0,)), ((), ())), preferred_element_type=F32)


def dot_nt(a, b):
    return lax.dot_general(a, b, (((1,), (1,)), ((), ())), preferred_element_type=F32)


def normed(h):
    wide = h.astype(F32)
    scale = lax.rsqrt(jnp.mean(wide * wide, -1, keepdims=True) + 1e-6)
    return (wide * scale).astype(BF)


def pipelined(count, parts, *stages):
    size = T // count // parts

    def one(b, c):
        rows = [pl.ds(pl.multiple_of(b * (size * parts) + p * size, size), size) for p in range(parts)]
        values = [()] * parts
        for step in range(parts + len(stages) - 1):
            for k, stage in enumerate(stages):
                p = step - k
                if 0 <= p < parts:
                    out = stage(rows[p], *values[p])
                    values[p] = out if isinstance(out, tuple) else (out,)
        return c

    lax.fori_loop(0, count, one, 0)


def forward_kernel(x_ref, dy_ref, wg_ref, wu_ref, wd_ref, gate_ref, up_ref, h1_ref, a1_ref, a0t_ref, a1t_ref, dyt_ref, a0, acc, stage, sem):
    j = pl.program_id(0)

    @pl.when(j == 0)
    def _():
        def one(b, c):
            rows = pl.ds(pl.multiple_of(b * TB, TB), TB)
            a = normed(x_ref[rows, :])
            a0[rows, :] = a
            acc[rows, :] = jnp.zeros((TB, D), F32)
            return c

        lax.fori_loop(0, T // TB, one, 0)

    def transposed(src, dst):
        def one(b, c):
            rows = pl.ds(pl.multiple_of(b * TB, TB), TB)
            stage[:, rows] = src[rows, :].T
            return c

        lax.fori_loop(0, T // TB, one, 0)
        copy = pltpu.make_async_copy(stage, dst, sem)
        copy.start()
        copy.wait()

    @pl.when(j == 1)
    def _():
        transposed(a0, a0t_ref)

    @pl.when(j == 2)
    def _():
        transposed(dy_ref, dyt_ref)

    def gate_up(rows):
        a = a0[rows, :]
        return dot(a, wg_ref[0]), dot(a, wu_ref[0])

    def hidden(rows, gate, up):
        gate_ref[0, rows, :] = gate
        up_ref[0, rows, :] = up
        return (gate * jax.nn.sigmoid(gate) * up).astype(BF)

    def down(rows, hid):
        acc[rows, :] += dot(hid, wd_ref[0])

    pipelined(T // FB, FB // FH, gate_up, hidden, down)

    @pl.when(j == NS - 1)
    def _():
        def one(b, c):
            rows = pl.ds(pl.multiple_of(b * TB, TB), TB)
            h1 = (x_ref[rows, :].astype(F32) + acc[rows, :].astype(BF).astype(F32)).astype(BF)
            h1_ref[rows, :] = h1
            a1_ref[rows, :] = normed(h1)
            return c

        lax.fori_loop(0, T // TB, one, 0)
        transposed(a1_ref, a1t_ref)


def forward(x, dy, wg, wu, wd):
    whole = pl.BlockSpec((T, D), lambda j: (0, 0))
    wide = pl.BlockSpec((1, T, SL), lambda j: (j, 0, 0))
    anyspec = pl.BlockSpec(memory_space=pl.ANY)
    return pl.pallas_call(
        forward_kernel,
        name="forward",
        grid=(NS,),
        in_specs=[
            whole,
            whole,
            pl.BlockSpec((1, D, SL), lambda j: (0, 0, j)),
            pl.BlockSpec((1, D, SL), lambda j: (0, 0, j)),
            pl.BlockSpec((1, SL, D), lambda j: (0, j, 0)),
        ],
        out_specs=[wide, wide, whole, whole, anyspec, anyspec, anyspec],
        out_shape=[
            jax.ShapeDtypeStruct((NS, T, SL), F32),
            jax.ShapeDtypeStruct((NS, T, SL), F32),
            jax.ShapeDtypeStruct((T, D), BF),
            jax.ShapeDtypeStruct((T, D), BF),
            jax.ShapeDtypeStruct((D, T), BF),
            jax.ShapeDtypeStruct((D, T), BF),
            jax.ShapeDtypeStruct((D, T), BF),
        ],
        scratch_shapes=[pltpu.VMEM((T, D), BF), pltpu.VMEM((T, D), F32), pltpu.VMEM((D, T), BF), pltpu.SemaphoreType.DMA],
        compiler_params=pltpu.CompilerParams(vmem_limit_bytes=VMEM_LIMIT),
        cost_estimate=pl.CostEstimate(flops=6 * T * D * FF, bytes_accessed=100_000_000, transcendentals=T * FF),
    )(x, dy, wg, wu, wd)


def backward_kernel(
    a1_ref, dy_ref, a1t_ref, dyt_ref, h1_ref, a0t_ref, gate_ref, up_ref, wg_ref, wu_ref, wd_ref,
    g1_ref, g0_ref,
    act, by, actt, byt, acc, hid, dgt, dup, wgb, wub, wdb,
    grad, s1, s2, sa0, ra0, sb0, rb0, sa1, ra1, sb1, rb1, sa2, ra2, sb2, rb2, cb, g0b,
    wsem, asem, lsem, send, recv,
):
    me = lax.axis_index("dp")
    xyz = (lax.div(me, 16), lax.rem(lax.div(me, 4), 4), lax.rem(me, 4))
    stride = (16, 4, 1)
    axes = [[(m + k) % 3 for k in range(3)] for m in range(3)]
    plus = [me + (lax.rem(xyz[d] + 1, 4) - xyz[d]) * stride[d] for d in range(3)]
    minus = [me + (lax.rem(xyz[d] + 3, 4) - xyz[d]) * stride[d] for d in range(3)]
    digit = [[xyz[d] for d in axes[m]] for m in range(3)]
    to = [[(plus[d], minus[d]) for d in axes[m]] for m in range(3)]

    def turn(c, k):
        return lax.rem(c + k, 4)

    def block(c, size):
        return pl.ds(pl.multiple_of(c * size, size), size)

    barrier = pltpu.get_barrier_semaphore()
    for d in range(3):
        for n in (plus[d], minus[d]):
            pl.semaphore_signal(barrier, inc=1, device_id={"dp": n}, device_id_type=MESH)
    pl.semaphore_wait(barrier, 6)

    HALF = (pl.ds(0, 128), pl.ds(128, 128))
    sas, ras, sbs, rbs = (sa0, sa1, sa2), (ra0, ra1, ra2), (sb0, sb1, sb2), (rb0, rb1, rb2)
    sizes = (256, 64, 16)

    def parts(r, s, m, k):
        slot = lax.rem(s, SLOTS)
        if r < 6:
            ph = r // 2
            send_buf, recv_buf = (sas[ph], ras[ph]) if r % 2 == 0 else (sbs[ph], rbs[ph])
            return send_buf.at[slot, m, k], recv_buf.at[slot, m, k]
        cbm = cb.at[lax.rem(s, CB), m]
        ph = 2 - (r - 6) // 2
        c = digit[m][ph]
        if r % 2 == 1:
            c = turn(c, 3 if k == 0 else 1)
        rows = block(digit[m][1] * 4 + c, 16) if ph == 2 else block(c, sizes[ph])
        if ph == 0:
            out = g1_ref.at[m, s, rows]
            return (cbm, out) if r % 2 == 0 else (out.at[:, HALF[k]], out.at[:, HALF[k]])
        at = cbm.at[rows] if r % 2 == 0 else cbm.at[rows, HALF[k]]
        return at, at

    def copies(r, s):
        slot = lax.rem(s, SEMS)
        ph = r // 2 if r < 6 else 2 - (r - 6) // 2
        for m in range(3):
            for k in range(2):
                src, dst = parts(r, s, m, k)
                yield pltpu.make_async_remote_copy(
                    src_ref=src,
                    dst_ref=dst,
                    send_sem=send.at[r, slot, m, k],
                    recv_sem=recv.at[r, slot, m, k],
                    device_id={"dp": to[m][ph][k]},
                    device_id_type=MESH,
                )

    def own_copy(s, m):
        return pltpu.make_async_copy(
            cb.at[lax.rem(s, CB), m], g1_ref.at[m, s, block(digit[m][0], 256)], lsem.at[lax.rem(s, SEMS), m]
        )

    def total(ph, s):
        return grad.at[lax.rem(s, GRADS)] if ph == 0 else (s1, s2)[ph - 1].at[lax.rem(s, SLOTS)]

    def mine(ph, s, m):
        slot = lax.rem(s, SLOTS)
        rows = block(digit[m][ph], sizes[ph])
        return total(ph, s)[m, rows, :] + rbs[ph][slot, m, 0].astype(F32) + rbs[ph][slot, m, 1].astype(F32)

    def prepare(r, s):
        slot = lax.rem(s, SLOTS)
        if r > 0:
            for copy in copies(r - 1, s):
                copy.wait()
        for m in range(3):
            ph = r // 2
            if r in (2, 4):
                total(ph, s)[m] = mine(ph - 1, s, m)
            if r in (0, 2, 4):
                far = block(turn(digit[m][ph], 2), sizes[ph])
                for k in range(2):
                    sas[ph][slot, m, k] = total(ph, s)[m, far, HALF[k]].astype(BF)
            if r in (1, 3, 5):
                for k in range(2):
                    near = block(turn(digit[m][ph], 1 if k == 0 else 3), sizes[ph])
                    add, keep = HALF[k], HALF[1 - k]
                    sbs[ph][slot, m, k, :, add] = (total(ph, s)[m, near, add] + ras[ph][slot, m, k].astype(F32)).astype(BF)
                    sbs[ph][slot, m, k, :, keep] = total(ph, s)[m, near, keep].astype(BF)
            if r == 6:
                done = mine(2, s, m).astype(BF)

                @pl.when(s < NS + Q)
                def _():
                    cb[lax.rem(s, CB), m, block(digit[m][1] * 4 + digit[m][2], 16), :] = done

                @pl.when(s >= NS + Q)
                def _():
                    g0b[m, s - NS - Q] = done

            if r == NR:
                own_copy(s, m).wait()

    def start(r, s):
        for copy in copies(r, s):
            copy.start()
        if r == 10:
            for m in range(3):
                own_copy(s, m).start()

    def service(h):
        q1, r1 = lax.div(h, STEPS1), lax.rem(h, STEPS1)
        q0, r0 = lax.div(h, STEPS0), lax.rem(h, STEPS0)
        todo = []
        for r in (2, 3, 4, 5, 0, 1, 6, 7, 8, 9, 10, 11, 12):
            from1, from0 = STEPS1 - 1 + OFF[r], START0 + STEPS0 - 1 + OFF[r]
            one = (r1 == from1 % STEPS1) & (h >= from1) & (h < from1 + STEPS1 * NS)

            def zero(count):
                return (r0 == from0 % STEPS0) & (h >= from0) & (h < from0 + STEPS0 * count)

            s = jnp.where(h >= from0, NS + q0 - from0 // STEPS0, q1 - from1 // STEPS1)
            prepared = one | zero(NS if r <= 6 else Q)
            todo.append((r, s, prepared, one | zero(Q) if r == 6 else prepared))
        for r, s, prepared, _ in todo:
            pl.when(prepared)(functools.partial(prepare, r, s))
        for r, s, _, sent in todo:
            if r < NR:
                pl.when(sent)(functools.partial(start, r, s))

    def weights(i):
        slot = lax.rem(i, 2)
        first = i < NS
        j = lax.rem(i, NS)
        columns = block(j, SL)
        down = pltpu.make_async_copy(wd_ref.at[jnp.where(first, 1, 0), columns, :], wdb.at[slot], wsem.at[slot, 0])
        one = [
            pltpu.make_async_copy(wg_ref.at[1, :, columns], wgb.at[slot], wsem.at[slot, 1]),
            pltpu.make_async_copy(wu_ref.at[1, :, columns], wub.at[slot], wsem.at[slot, 2]),
        ]
        zero = [
            pltpu.make_async_copy(gate_ref.at[j], acc.at[2 * slot], wsem.at[slot, 1]),
            pltpu.make_async_copy(up_ref.at[j], acc.at[2 * slot + 1], wsem.at[slot, 2]),
        ]
        return down, one, zero

    loads = [
        pltpu.make_async_copy(a1_ref, act, asem.at[0]),
        pltpu.make_async_copy(dy_ref, by, asem.at[1]),
        pltpu.make_async_copy(a1t_ref, actt, asem.at[2]),
        pltpu.make_async_copy(dyt_ref, byt, asem.at[3]),
    ]
    down, one, _ = weights(0)
    for copy in [down, *one, *loads]:
        copy.start()

    def clear(b, c):
        rows = block(b, TB)
        for n in range(4):
            acc[n, rows, :] = jnp.zeros((TB, SL), F32)
        return c

    lax.fori_loop(0, T // TB, clear, 0)
    loads[0].wait()
    loads[1].wait()
    h1_load = pltpu.make_async_copy(h1_ref, act, asem.at[0])
    a0t_load = pltpu.make_async_copy(a0t_ref, actt, asem.at[2])

    def second_layer(i, part):
        slot = lax.rem(i, 2)

        @pl.when(part == 0)
        def _():
            down, one, _ = weights(i)
            for copy in [down, *one]:
                copy.wait()

            @pl.when(i + 1 < NS)
            def _():
                down, one, _ = weights(i + 1)
                for copy in [down, *one]:
                    copy.start()

        def products(rows):
            a = act[rows, :]
            return dot(a, wgb[slot]), dot(a, wub[slot]), dot_nt(by[rows, :], wdb[slot])

        def elements(rows, gate, up, by_hid):
            by_hid = by_hid.astype(BF).astype(F32)
            sig = jax.nn.sigmoid(gate)
            silu = gate * sig
            hid[rows, :] = (silu * up).astype(BF)
            by_up = (by_hid * silu).astype(BF)
            by_gate = (by_hid * up * (sig * (1.0 + gate * (1.0 - sig)))).astype(BF)
            dup[rows, :] = by_up
            dgt[rows, :] = by_gate
            return by_gate, by_up

        def back(rows, by_gate, by_up):
            for n in range(4):
                acc[n, rows, :] += dot_nt(by_gate, wgb[slot, pl.ds(n * SL, SL), :]) + dot_nt(by_up, wub[slot, pl.ds(n * SL, SL), :])

        half = T // 2
        count = half // H
        rows = [pl.ds(pl.multiple_of(part * half + p * H, H), H) for p in range(count)]
        d, e = [None] * count, [None] * count
        for p in range(count + 2):
            if p < count:
                d[p] = products(rows[p])
            if 0 <= p - 1 < count:
                e[p - 1] = elements(rows[p - 1], *d[p - 1])
            if 0 <= p - 2 < count:
                back(rows[p - 2], *e[p - 2])

    def between(part):
        @pl.when(part == 0)
        def _():
            h1_load.wait()
            a0t_load.start()
            weights(NS)[0].start()

        quarter = T // MID

        def tokens(b, c):
            rows = pl.ds(pl.multiple_of(part * quarter + b * H, H), H)
            wide = act[rows, :].astype(F32)
            scale = lax.rsqrt(jnp.mean(wide * wide, -1, keepdims=True) + 1e-6)
            da = jnp.concatenate([acc[n, rows, :] for n in range(4)], axis=1).astype(BF).astype(F32)
            t = jnp.mean(da * wide, -1, keepdims=True)
            dwide = (da * scale - wide * (scale * scale * scale * t)).astype(BF)
            by_h = (by[rows, :].astype(F32) + dwide.astype(F32)).astype(BF)
            by[rows, :] = by_h
            byt[:, rows] = by_h.T
            return c

        lax.fori_loop(0, quarter // H, tokens, 0)

        @pl.when(part == MID - 1)
        def _():
            for copy in weights(NS)[2]:
                copy.start()
            a0t_load.wait()

    def first_layer(i):
        slot = lax.rem(i, 2)
        down, _, zero = weights(i)
        for copy in [down, *zero]:
            copy.wait()

        @pl.when(i + 1 < 2 * NS)
        def _():
            down, _, zero = weights(i + 1)
            for copy in [down, *zero]:
                copy.start()

        def products(rows):
            return dot_nt(by[rows, :], wdb[slot])

        def elements(rows, by_hid):
            gate = acc[2 * slot, rows, :]
            up = acc[2 * slot + 1, rows, :]
            by_hid = by_hid.astype(BF).astype(F32)
            sig = jax.nn.sigmoid(gate)
            silu = gate * sig
            hid[rows, :] = (silu * up).astype(BF)
            dup[rows, :] = (by_hid * silu).astype(BF)
            dgt[rows, :] = (by_hid * up * (sig * (1.0 + gate * (1.0 - sig)))).astype(BF)

        pipelined(T // TB, TB // H, products, elements)

    def gradient(s, m):
        left, right = ((actt, dgt), (actt, dup), (byt, hid))[m]
        grad[lax.rem(s, GRADS), m] = dot(left[...], right[...])

    def step(h, c):
        in1 = h < STEPS1 * NS
        in0 = (h >= START0) & (h < START0 + STEPS0 * NS)
        h0 = h - START0
        s = jnp.where(in1, lax.div(h, STEPS1), NS + lax.div(h0, STEPS0))
        part = jnp.where(in1, lax.rem(h, STEPS1), lax.rem(h0, STEPS0))

        @pl.when(in1 & (part < 2))
        def _():
            second_layer(s, part)

        @pl.when(h == 2)
        def _():
            loads[2].wait()
            loads[3].wait()

        @pl.when(h == STEPS1 * NS - 1)
        def _():
            h1_load.start()

        @pl.when((h >= STEPS1 * NS) & (h < START0))
        def _():
            between(h - STEPS1 * NS)

        @pl.when(in0 & (part == 0))
        def _():
            first_layer(s)

        @pl.when((in1 & (part == STEPS1 - 2)) | (in0 & (part == 0)))
        def _():
            gradient(s, 0)

        @pl.when((in1 & (part == STEPS1 - 1)) | (in0 & (part == 1)))
        def _():
            gradient(s, 1)
            gradient(s, 2)

        service(h)
        return c

    last = max(START0 + STEPS0 * NS + OFF[6], STEPS1 * NS + OFF[NR], START0 + STEPS0 * Q + OFF[NR])
    lax.fori_loop(0, last, step, 0)
    out = pltpu.make_async_copy(g0b, g0_ref, asem.at[0])
    out.start()
    out.wait()


def backward(a1, dy, a1t, dyt, h1, a0t, gate, up, wg, wu, wd):
    anyspec = pl.BlockSpec(memory_space=pl.ANY)
    V = pltpu.VMEM
    DMA = pltpu.SemaphoreType.DMA
    return pl.pallas_call(
        backward_kernel,
        name="backward",
        in_specs=[anyspec] * 11,
        out_specs=[anyspec] * 2,
        out_shape=[jax.ShapeDtypeStruct((3, NS + Q, D, SL), BF), jax.ShapeDtypeStruct((3, NS - Q, 16, SL), BF)],
        scratch_shapes=[
            V((T, D), BF), V((T, D), BF), V((D, T), BF), V((D, T), BF), V((4, T, SL), F32),
            V((T, SL), BF), V((T, SL), BF), V((T, SL), BF),
            V((2, D, SL), BF), V((2, D, SL), BF), V((2, SL, D), BF),
            V((GRADS, 3, D, SL), F32), V((SLOTS, 3, 256, SL), F32), V((SLOTS, 3, 64, SL), F32),
            *[V((SLOTS, 3, 2, size, width), BF) for size in (256, 64, 16) for width in (128, 128, SL, SL)],
            V((CB, 3, 256, SL), BF), V((3, NS - Q, 16, SL), BF),
            DMA((2, 3)), DMA((4,)), DMA((SEMS, 3)), DMA((NR, SEMS, 3, 2)), DMA((NR, SEMS, 3, 2)),
        ],
        compiler_params=pltpu.CompilerParams(vmem_limit_bytes=VMEM_LIMIT, collective_id=0, has_side_effects=True),
        cost_estimate=pl.CostEstimate(flops=24 * T * D * FF, bytes_accessed=150_000_000, transcendentals=2 * T * FF),
    )(a1, dy, a1t, dyt, h1, a0t, gate, up, wg, wu, wd)


def adam_kernel(gathered, *refs):
    ins, rest = refs[:12], refs[12:]
    if gathered:
        rest = rest[9:]
    outs, rest = rest[:9], rest[9:]
    for m in range(3):
        w_ref, m_ref, v_ref, g_ref = ins[m], ins[3 + m], ins[6 + m], ins[9 + m]
        w_out, m_out, v_out = outs[m], outs[3 + m], outs[6 + m]

        def take(at, g):
            g = g.astype(F32)
            w = w_ref[at].astype(F32)
            mean = 0.9 * m_ref[at] + 0.1 * g
            var = 0.95 * v_ref[at] + 0.05 * g * g
            w_out[at] = (w - 0.02 * (mean * lax.rsqrt(var + 1e-8) + 0.1 * w)).astype(BF)
            m_out[at] = mean
            v_out[at] = var

        if gathered:
            whole = rest[0]
            for n in range(64 // CUT):
                digits = (n // 16, n // 4 % 4, n % 4)
                x, y, z = (digits[(d - m) % 3] for d in range(3))
                whole[n * 16 : n * 16 + 16, :] = g_ref[x, y, z, 0, 0]
            look = lambda rows: whole[rows, :]
        else:
            look = lambda rows: g_ref[0, 0, rows, :]

        if m < 2:

            def one(b, c):
                rows = pl.ds(pl.multiple_of(b * 64, 64), 64)
                take((0, rows, slice(None)), look(rows))
                return c

            lax.fori_loop(0, D // CUT // 64, one, 0)
        else:

            def one(b, c):
                rows = pl.ds(pl.multiple_of(b * 128, 128), 128)
                take((0, slice(None), rows), look(rows).T)
                return c

            lax.fori_loop(0, D // CUT // 128, one, 0)


def adam(first, count, weights, means, variances, gradients, so_far=None):
    rows = D // CUT

    def place(j):
        s = first + j // CUT
        return jnp.where(s < NS, 1, 0), jnp.where(s < NS, s, s - NS), j % CUT

    def at_wide(j):
        layer, column, row = place(j)
        return layer, row, column

    wide = pl.BlockSpec((1, rows, SL), at_wide)
    tall = pl.BlockSpec((1, SL, rows), place)
    mine = [wide, wide, tall]
    gathered = so_far is not None
    if gathered:
        gradients = gradients.reshape(4, 4, 4, *gradients.shape[1:])

        def spec(m):
            return pl.BlockSpec(
                tuple(4 // CUT if d == m else 4 for d in range(3)) + (1, 1, 16, SL),
                lambda j: tuple(j % CUT if d == m else 0 for d in range(3)) + (m, j // CUT, 0, 0),
            )

    else:

        def spec(m):
            return pl.BlockSpec((1, 1, rows, SL), lambda j: (m, j // CUT, j % CUT, 0))

    shapes = [jax.ShapeDtypeStruct(a.shape, a.dtype) for a in (*weights, *means, *variances)]
    return pl.pallas_call(
        functools.partial(adam_kernel, gathered),
        name="adamw_rest" if gathered else "adamw",
        grid=(count * CUT,),
        in_specs=mine * 3 + [spec(m) for m in range(3)] + ([pl.BlockSpec(memory_space=pl.ANY)] * 9 if gathered else []),
        out_specs=mine * 3,
        out_shape=shapes,
        input_output_aliases={12 + k: k for k in range(9)} if gathered else {},
        scratch_shapes=[pltpu.VMEM((rows, SL), BF)] if gathered else [],
        compiler_params=pltpu.CompilerParams(vmem_limit_bytes=VMEM_LIMIT),
        cost_estimate=pl.CostEstimate(flops=10**10, bytes_accessed=66 * D * SL * count, transcendentals=3 * D * SL * count),
    )(*weights, *means, *variances, *[gradients] * 3, *(so_far or ()))


def solution(mesh):
    def step(x, dy, *arrays):
        x, dy = x[0], dy[0]
        weights, means, variances = (arrays[k : k + 3] for k in (0, 3, 6))
        gate, up, h1, a1, a0t, a1t, dyt = forward(x, dy, *weights)
        g1, g0 = backward(a1, dy, a1t, dyt, h1, a0t, gate, up, *weights)
        g0 = lax.all_gather(g0, "dp", axis=0)
        new = adam(0, NS + Q, weights, means, variances, g1)
        return tuple(adam(NS + Q, NS - Q, weights, means, variances, g0, new))

    return jax.shard_map(
        step,
        mesh=mesh,
        in_specs=(P(("rep", "dp"), None, None),) * 2 + (P(None, None, None),) * 9,
        out_specs=(P("rep", None, None),) * 9,
        check_vma=False,
    )
```

```python
import functools

import jax
import jax.numpy as jnp
from jax import lax
from jax.experimental import pallas as pl
from jax.experimental.pallas import tpu as pltpu
from jax.sharding import PartitionSpec as P

T, D, FF, SL = 2048, 1024, 3328, 256
NS = FF // SL
TB = 512
H = 256
FH = 512
PIECES = 8
F32, BF = jnp.float32, jnp.bfloat16
MESH = pl.DeviceIdType.MESH
VMEM_LIMIT = 66_900_000

STEPS1, MID, STEPS0 = 4, 4, 2
START0 = STEPS1 * NS + MID
OFF = (0, 2, 5, 7, 9, 11, 13, 15, 17, 20, 23, 29, 32)
NR = 12
SLOTS, SEMS, CB = 4, 4, 8
Q = 3
CUT = 1


def dot(a, b):
    return lax.dot_general(a, b, (((1,), (0,)), ((), ())), preferred_element_type=F32)


def dot_nt(a, b):
    return lax.dot_general(a, b, (((1,), (1,)), ((), ())), preferred_element_type=F32)


def normed(h):
    wide = h.astype(F32)
    scale = lax.rsqrt(jnp.mean(wide * wide, -1, keepdims=True) + 1e-6)
    return (wide * scale).astype(BF)


def pipelined(count, parts, *stages):
    size = T // count // parts

    def one(b, c):
        rows = [pl.ds(pl.multiple_of(b * (size * parts) + p * size, size), size) for p in range(parts)]
        values = [()] * parts
        for step in range(parts + len(stages) - 1):
            for k, stage in enumerate(stages):
                p = step - k
                if 0 <= p < parts:
                    out = stage(rows[p], *values[p])
                    values[p] = out if isinstance(out, tuple) else (out,)
        return c

    lax.fori_loop(0, count, one, 0)


def step_kernel(
    x_ref, dy_ref, wg_ref, wu_ref, wd_ref,
    g1_ref, g0_ref, gate_ref, up_ref, h1_ref, a0t_ref,
    act, by, actt, byt, acc, hid, dgt, dup, wgb, wub, wdb,
    grad, s1, s2, sa0, ra0, sb0, rb0, sa1, ra1, sb1, rb1, sa2, ra2, sb2, rb2, cb, g0b,
    wsem, asem, osem, lsem, send, recv,
):
    me = lax.axis_index("dp")
    xyz = (lax.div(me, 16), lax.rem(lax.div(me, 4), 4), lax.rem(me, 4))
    stride = (16, 4, 1)
    axes = [[(m + k) % 3 for k in range(3)] for m in range(3)]
    plus = [me + (lax.rem(xyz[d] + 1, 4) - xyz[d]) * stride[d] for d in range(3)]
    minus = [me + (lax.rem(xyz[d] + 3, 4) - xyz[d]) * stride[d] for d in range(3)]
    digit = [[xyz[d] for d in axes[m]] for m in range(3)]
    to = [[(plus[d], minus[d]) for d in axes[m]] for m in range(3)]

    def turn(c, k):
        return lax.rem(c + k, 4)

    def block(c, size):
        return pl.ds(pl.multiple_of(c * size, size), size)

    barrier = pltpu.get_barrier_semaphore()
    for d in range(3):
        for n in (plus[d], minus[d]):
            pl.semaphore_signal(barrier, inc=1, device_id={"dp": n}, device_id_type=MESH)

    HALF = (pl.ds(0, 128), pl.ds(128, 128))
    sas, ras, sbs, rbs = (sa0, sa1, sa2), (ra0, ra1, ra2), (sb0, sb1, sb2), (rb0, rb1, rb2)
    sizes = (256, 64, 16)

    def parts(r, s, m, k):
        slot = lax.rem(s, SLOTS)
        if r < 6:
            ph = r // 2
            send_buf, recv_buf = (sas[ph], ras[ph]) if r % 2 == 0 else (sbs[ph], rbs[ph])
            return send_buf.at[slot, m, k], recv_buf.at[slot, m, k]
        cbm = cb.at[lax.rem(s, CB), m]
        ph = 2 - (r - 6) // 2
        c = digit[m][ph]
        if r % 2 == 1:
            c = turn(c, 3 if k == 0 else 1)
        rows = block(digit[m][1] * 4 + c, 16) if ph == 2 else block(c, sizes[ph])
        if ph == 0:
            out = g1_ref.at[m, s, rows]
            return (cbm, out) if r % 2 == 0 else (out.at[:, HALF[k]], out.at[:, HALF[k]])
        at = cbm.at[rows] if r % 2 == 0 else cbm.at[rows, HALF[k]]
        return at, at

    def copies(r, s):
        slot = lax.rem(s, SEMS)
        ph = r // 2 if r < 6 else 2 - (r - 6) // 2
        for m in range(3):
            for k in range(2):
                src, dst = parts(r, s, m, k)
                yield pltpu.make_async_remote_copy(
                    src_ref=src,
                    dst_ref=dst,
                    send_sem=send.at[r, slot, m, k],
                    recv_sem=recv.at[r, slot, m, k],
                    device_id={"dp": to[m][ph][k]},
                    device_id_type=MESH,
                )

    def own_copy(s, m):
        return pltpu.make_async_copy(
            cb.at[lax.rem(s, CB), m], g1_ref.at[m, s, block(digit[m][0], 256)], lsem.at[lax.rem(s, SEMS), m]
        )

    def total(ph, s):
        return grad.at[pl.ds(pl.multiple_of(4 * lax.rem(s, 2), 4), 4)] if ph == 0 else (s1, s2)[ph - 1].at[lax.rem(s, SLOTS)]

    def mine(ph, s, m):
        slot = lax.rem(s, SLOTS)
        rows = block(digit[m][ph], sizes[ph])
        so_far = s1[slot, m] if ph == 0 else total(ph, s)[m, rows, :]
        return so_far + rbs[ph][slot, m, 0].astype(F32) + rbs[ph][slot, m, 1].astype(F32)

    def prepare(r, s):
        slot = lax.rem(s, SLOTS)
        if r > 0:
            for copy in copies(r - 1, s):
                copy.wait()
        for m in range(3):
            ph = r // 2
            if r in (2, 4):
                total(ph, s)[m] = mine(ph - 1, s, m)
            if r in (0, 2, 4):
                far = block(turn(digit[m][ph], 2), sizes[ph])
                for k in range(2):
                    sas[ph][slot, m, k] = total(ph, s)[m, far, HALF[k]].astype(BF)
            if r in (1, 3, 5):
                for k in range(2):
                    near = block(turn(digit[m][ph], 1 if k == 0 else 3), sizes[ph])
                    add, keep = HALF[k], HALF[1 - k]
                    sbs[ph][slot, m, k, :, add] = (total(ph, s)[m, near, add] + ras[ph][slot, m, k].astype(F32)).astype(BF)
                    sbs[ph][slot, m, k, :, keep] = total(ph, s)[m, near, keep].astype(BF)
            if r == 1:
                s1[slot, m] = total(0, s)[m, block(digit[m][0], 256), :]
            if r == 6:
                done = mine(2, s, m).astype(BF)

                @pl.when(s < NS + Q)
                def _():
                    cb[lax.rem(s, CB), m, block(digit[m][1] * 4 + digit[m][2], 16), :] = done

                @pl.when(s >= NS + Q)
                def _():
                    g0b[m, s - NS - Q] = done

            if r == NR:
                own_copy(s, m).wait()

    def start(r, s):
        for copy in copies(r, s):
            copy.start()
        if r == 10:
            for m in range(3):
                own_copy(s, m).start()

    def service(h):
        q1, r1 = lax.div(h, STEPS1), lax.rem(h, STEPS1)
        q0, r0 = lax.div(h, STEPS0), lax.rem(h, STEPS0)

        def some(parity):
            todo = []
            for r in (2, 3, 4, 5, 0, 1, 6, 7, 8, 9, 10, 11, 12):
                from1, from0 = STEPS1 - 1 + OFF[r], START0 + STEPS0 - 1 + OFF[r]
                if from1 % 2 != parity:
                    continue
                one = (r1 == from1 % STEPS1) & (h >= from1) & (h < from1 + STEPS1 * NS)

                def zero(count):
                    return (r0 == from0 % STEPS0) & (h >= from0) & (h < from0 + STEPS0 * count)

                s = jnp.where(h >= from0, NS + q0 - from0 // STEPS0, q1 - from1 // STEPS1)
                prepared = one | zero(NS if r <= 6 else Q)
                todo.append((r, s, prepared, one | zero(Q) if r == 6 else prepared))
            for r, s, prepared, _ in todo:
                if r <= 6:
                    pl.when(prepared)(functools.partial(prepare, r, s))
            for r, s, _, sent in todo:

                @pl.when(sent)
                def _():
                    if r > 6:
                        prepare(r, s)
                    if r < NR:
                        start(r, s)

        for parity in range(2):
            pl.when(lax.rem(h, 2) == parity)(functools.partial(some, parity))

    def weights(i):
        slot = lax.rem(i, 2)
        first = i < NS
        j = lax.rem(i, NS)
        columns = block(j, SL)
        down = pltpu.make_async_copy(wd_ref.at[jnp.where(first, 1, 0), columns, :], wdb.at[slot], wsem.at[slot, 0])
        one = [
            pltpu.make_async_copy(wg_ref.at[1, :, columns], wgb.at[slot], wsem.at[slot, 1]),
            pltpu.make_async_copy(wu_ref.at[1, :, columns], wub.at[slot], wsem.at[slot, 2]),
        ]
        zero = [
            pltpu.make_async_copy(gate_ref.at[j], acc.at[2 * slot], wsem.at[slot, 1]),
            pltpu.make_async_copy(up_ref.at[j], acc.at[2 * slot + 1], wsem.at[slot, 2]),
        ]
        return down, one, zero

    def first_weights(j):
        slot, columns = lax.rem(j, 2), block(j, SL)
        return [
            pltpu.make_async_copy(wg_ref.at[0, :, columns], wgb.at[slot], wsem.at[slot, 0]),
            pltpu.make_async_copy(wu_ref.at[0, :, columns], wub.at[slot], wsem.at[slot, 1]),
            pltpu.make_async_copy(wd_ref.at[0, columns, :], wdb.at[slot], wsem.at[slot, 2]),
        ]

    def kept(j):
        slot = lax.rem(j, 2)
        return [
            pltpu.make_async_copy(grad.at[4 * slot + 2 * k + half], ref.at[j, pl.ds(half * D, D)], osem.at[slot, k, half])
            for k, ref in enumerate((gate_ref, up_ref))
            for half in range(2)
        ]

    x_load = pltpu.make_async_copy(x_ref, act, asem.at[0])
    dy_load = pltpu.make_async_copy(dy_ref, by, asem.at[1])
    for copy in [x_load, *first_weights(0), dy_load]:
        copy.start()

    def clear(rows):
        for n in range(4):
            acc[n, rows, :] = jnp.zeros((TB, SL), F32)

    x_load.wait()

    def enter(b, c):
        rows = block(b, TB)
        act[rows, :] = normed(act[rows, :])
        clear(rows)
        return c

    lax.fori_loop(0, T // TB, enter, 0)
    dy_load.wait()

    def forward(j, c):
        slot = lax.rem(j, 2)
        for copy in first_weights(j):
            copy.wait()

        @pl.when(j + 1 < NS)
        def _():
            for copy in first_weights(j + 1):
                copy.start()

        @pl.when(j >= 2)
        def _():
            for copy in kept(j - 2):
                copy.wait()

        piece = block(jnp.minimum(j, PIECES - 1), T // PIECES)
        actt[:, piece] = act[piece, :].T
        byt[:, piece] = by[piece, :].T

        def gate_up(p):
            a = act[p * FH : p * FH + FH, :]
            return dot(a, wgb[slot]), dot(a, wub[slot])

        def hidden(p, gate, up):
            half, at = divmod(p * FH, D)
            grad[4 * slot + half, at : at + FH, :] = gate
            grad[4 * slot + 2 + half, at : at + FH, :] = up
            return ((gate * jax.nn.sigmoid(gate) * up).astype(BF),)

        def down(p, hidden):
            for n in range(4):
                acc[n, p * FH : p * FH + FH, :] += dot(hidden, wdb[slot, :, n * SL : n * SL + SL])

        parts = T // FH
        values = [()] * parts
        for at in range(parts + 2):
            for k, work in enumerate((gate_up, hidden, down)):
                if 0 <= at - k < parts:
                    values[at - k] = work(at - k, *values[at - k])
        for copy in kept(j):
            copy.start()
        return c

    lax.fori_loop(0, NS, forward, 0)
    a0t_keep = pltpu.make_async_copy(actt, a0t_ref, asem.at[2])
    again = pltpu.make_async_copy(x_ref, act, asem.at[0])
    a0t_keep.start()
    again.start()
    down, one, _ = weights(0)
    for copy in [down, *one]:
        copy.start()
    for copy in [*kept(NS - 2), *kept(NS - 1)]:
        copy.wait()
    a0t_keep.wait()
    again.wait()
    h1_keep = pltpu.make_async_copy(act, h1_ref, asem.at[1])

    def leave(b, c):
        rows = block(b, TB)
        added = jnp.concatenate([acc[n, rows, :] for n in range(4)], axis=1).astype(BF)
        act[rows, :] = (act[rows, :].astype(F32) + added.astype(F32)).astype(BF)
        clear(rows)
        return c

    lax.fori_loop(0, T // TB, leave, 0)
    h1_keep.start()
    h1_keep.wait()

    def enter_second(b, c):
        rows = block(b, TB)
        a1 = normed(act[rows, :])
        act[rows, :] = a1
        actt[:, rows] = a1.T
        return c

    lax.fori_loop(0, T // TB, enter_second, 0)
    pl.semaphore_wait(barrier, 6)
    h1_load = pltpu.make_async_copy(h1_ref, act, asem.at[0])
    a0t_load = pltpu.make_async_copy(a0t_ref, actt, asem.at[2])

    def second_layer(i, part):
        slot = lax.rem(i, 2)

        @pl.when(part == 0)
        def _():
            down, one, _ = weights(i)
            for copy in [down, *one]:
                copy.wait()

            @pl.when(i + 1 < NS)
            def _():
                down, one, _ = weights(i + 1)
                for copy in [down, *one]:
                    copy.start()

        def products(rows):
            a = act[rows, :]
            return dot(a, wgb[slot]), dot(a, wub[slot]), dot_nt(by[rows, :], wdb[slot])

        def elements(rows, gate, up, by_hid):
            by_hid = by_hid.astype(BF).astype(F32)
            sig = jax.nn.sigmoid(gate)
            silu = gate * sig
            hid[rows, :] = (silu * up).astype(BF)
            by_up = (by_hid * silu).astype(BF)
            by_gate = (by_hid * up * (sig * (1.0 + gate * (1.0 - sig)))).astype(BF)
            dup[rows, :] = by_up
            dgt[rows, :] = by_gate
            return by_gate, by_up

        def back(rows, by_gate, by_up):
            for n in range(4):
                acc[n, rows, :] += dot_nt(by_gate, wgb[slot, pl.ds(n * SL, SL), :]) + dot_nt(by_up, wub[slot, pl.ds(n * SL, SL), :])

        half = T // 2
        count = half // H
        rows = [pl.ds(pl.multiple_of(part * half + p * H, H), H) for p in range(count)]
        d, e = [None] * count, [None] * count
        for p in range(count + 2):
            if p < count:
                d[p] = products(rows[p])
            if 0 <= p - 1 < count:
                e[p - 1] = elements(rows[p - 1], *d[p - 1])
            if 0 <= p - 2 < count:
                back(rows[p - 2], *e[p - 2])

    def between(part):
        @pl.when(part == 0)
        def _():
            h1_load.wait()
            a0t_load.start()
            weights(NS)[0].start()

        quarter = T // MID

        def tokens(b, c):
            rows = pl.ds(pl.multiple_of(part * quarter + b * H, H), H)
            wide = act[rows, :].astype(F32)
            scale = lax.rsqrt(jnp.mean(wide * wide, -1, keepdims=True) + 1e-6)
            da = jnp.concatenate([acc[n, rows, :] for n in range(4)], axis=1).astype(BF).astype(F32)
            t = jnp.mean(da * wide, -1, keepdims=True)
            dwide = (da * scale - wide * (scale * scale * scale * t)).astype(BF)
            by_h = (by[rows, :].astype(F32) + dwide.astype(F32)).astype(BF)
            by[rows, :] = by_h
            byt[:, rows] = by_h.T
            return c

        lax.fori_loop(0, quarter // H, tokens, 0)

        @pl.when(part == MID - 1)
        def _():
            for copy in weights(NS)[2]:
                copy.start()
            a0t_load.wait()

    def first_layer(i):
        slot = lax.rem(i, 2)
        down, _, zero = weights(i)
        for copy in [down, *zero]:
            copy.wait()

        @pl.when(i + 1 < 2 * NS)
        def _():
            down, _, zero = weights(i + 1)
            for copy in [down, *zero]:
                copy.start()

        def products(rows):
            return dot_nt(by[rows, :], wdb[slot])

        def elements(rows, by_hid):
            gate = acc[2 * slot, rows, :]
            up = acc[2 * slot + 1, rows, :]
            by_hid = by_hid.astype(BF).astype(F32)
            sig = jax.nn.sigmoid(gate)
            silu = gate * sig
            hid[rows, :] = (silu * up).astype(BF)
            dup[rows, :] = (by_hid * silu).astype(BF)
            dgt[rows, :] = (by_hid * up * (sig * (1.0 + gate * (1.0 - sig)))).astype(BF)

        pipelined(T // TB, TB // H, products, elements)

    def gradient(s, m):
        left, right = ((actt, dgt), (actt, dup), (byt, hid))[m]
        grad[4 * lax.rem(s, 2) + m] = dot(left[...], right[...])

    def step(h, c):
        in1 = h < STEPS1 * NS
        in0 = (h >= START0) & (h < START0 + STEPS0 * NS)
        h0 = h - START0
        s = jnp.where(in1, lax.div(h, STEPS1), NS + lax.div(h0, STEPS0))
        part = jnp.where(in1, lax.rem(h, STEPS1), lax.rem(h0, STEPS0))

        @pl.when(in1 & (part < 2))
        def _():
            second_layer(s, part)

        @pl.when(h == STEPS1 * NS - 1)
        def _():
            h1_load.start()

        @pl.when((h >= STEPS1 * NS) & (h < START0))
        def _():
            between(h - STEPS1 * NS)

        @pl.when(in0 & (part == 0))
        def _():
            first_layer(s)

        @pl.when((in1 & (part == STEPS1 - 2)) | (in0 & (part == 0)))
        def _():
            gradient(s, 0)

        @pl.when((in1 & (part == STEPS1 - 1)) | (in0 & (part == 1)))
        def _():
            gradient(s, 1)
            gradient(s, 2)

        service(h)
        return c

    last = max(START0 + STEPS0 * NS + OFF[6], STEPS1 * NS + OFF[NR], START0 + STEPS0 * Q + OFF[NR])
    lax.fori_loop(0, last, step, 0)
    out = pltpu.make_async_copy(g0b, g0_ref, asem.at[0])
    out.start()
    out.wait()


def gradients(x, dy, wg, wu, wd):
    anyspec = pl.BlockSpec(memory_space=pl.ANY)
    V = pltpu.VMEM
    DMA = pltpu.SemaphoreType.DMA
    return pl.pallas_call(
        step_kernel,
        name="gradients",
        in_specs=[anyspec] * 5,
        out_specs=[anyspec] * 6,
        out_shape=[
            jax.ShapeDtypeStruct((3, NS + Q, D, SL), BF),
            jax.ShapeDtypeStruct((3, NS - Q, 16, SL), BF),
            jax.ShapeDtypeStruct((NS, T, SL), F32),
            jax.ShapeDtypeStruct((NS, T, SL), F32),
            jax.ShapeDtypeStruct((T, D), BF),
            jax.ShapeDtypeStruct((D, T), BF),
        ],
        scratch_shapes=[
            V((T, D), BF), V((T, D), BF), V((D, T), BF), V((D, T), BF), V((4, T, SL), F32),
            V((T, SL), BF), V((T, SL), BF), V((T, SL), BF),
            V((2, D, SL), BF), V((2, D, SL), BF), V((2, SL, D), BF),
            V((8, D, SL), F32), V((SLOTS, 3, 256, SL), F32), V((SLOTS, 3, 64, SL), F32),
            *[V((SLOTS, 3, 2, size, width), BF) for size in (256, 64, 16) for width in (128, 128, SL, SL)],
            V((CB, 3, 256, SL), BF), V((3, NS - Q, 16, SL), BF),
            DMA((2, 3)), DMA((4,)), DMA((2, 2, 2)), DMA((SEMS, 3)), DMA((NR, SEMS, 3, 2)), DMA((NR, SEMS, 3, 2)),
        ],
        compiler_params=pltpu.CompilerParams(vmem_limit_bytes=VMEM_LIMIT, collective_id=0, has_side_effects=True),
        cost_estimate=pl.CostEstimate(flops=30 * T * D * FF, bytes_accessed=250_000_000, transcendentals=3 * T * FF),
    )(x, dy, wg, wu, wd)[:2]


def adam_kernel(gathered, *refs):
    ins, rest = refs[:12], refs[12:]
    if gathered:
        rest = rest[9:]
    outs, rest = rest[:9], rest[9:]
    for m in range(3):
        w_ref, m_ref, v_ref, g_ref = ins[m], ins[3 + m], ins[6 + m], ins[9 + m]
        w_out, m_out, v_out = outs[m], outs[3 + m], outs[6 + m]

        def take(at, g):
            g = g.astype(F32)
            w = w_ref[at].astype(F32)
            mean = 0.9 * m_ref[at] + 0.1 * g
            var = 0.95 * v_ref[at] + 0.05 * g * g
            w_out[at] = (w - 0.02 * (mean * lax.rsqrt(var + 1e-8) + 0.1 * w)).astype(BF)
            m_out[at] = mean
            v_out[at] = var

        if gathered:
            whole = rest[0]
            for n in range(64 // CUT):
                digits = (n // 16, n // 4 % 4, n % 4)
                x, y, z = (digits[(d - m) % 3] for d in range(3))
                whole[n * 16 : n * 16 + 16, :] = g_ref[x, y, z, 0, 0]
            look = lambda rows: whole[rows, :]
        else:
            look = lambda rows: g_ref[0, 0, rows, :]

        if m < 2:

            def one(b, c):
                rows = pl.ds(pl.multiple_of(b * 64, 64), 64)
                take((0, rows, slice(None)), look(rows))
                return c

            lax.fori_loop(0, D // CUT // 64, one, 0)
        else:

            def one(b, c):
                rows = pl.ds(pl.multiple_of(b * 128, 128), 128)
                take((0, slice(None), rows), look(rows).T)
                return c

            lax.fori_loop(0, D // CUT // 128, one, 0)


def adam(first, count, weights, means, variances, gradients, so_far=None):
    rows = D // CUT

    def place(j):
        s = first + j // CUT
        return jnp.where(s < NS, 1, 0), jnp.where(s < NS, s, s - NS), j % CUT

    def at_wide(j):
        layer, column, row = place(j)
        return layer, row, column

    wide = pl.BlockSpec((1, rows, SL), at_wide)
    tall = pl.BlockSpec((1, SL, rows), place)
    mine = [wide, wide, tall]
    gathered = so_far is not None
    if gathered:
        gradients = gradients.reshape(4, 4, 4, *gradients.shape[1:])

        def spec(m):
            return pl.BlockSpec(
                tuple(4 // CUT if d == m else 4 for d in range(3)) + (1, 1, 16, SL),
                lambda j: tuple(j % CUT if d == m else 0 for d in range(3)) + (m, j // CUT, 0, 0),
            )

    else:

        def spec(m):
            return pl.BlockSpec((1, 1, rows, SL), lambda j: (m, j // CUT, j % CUT, 0))

    shapes = [jax.ShapeDtypeStruct(a.shape, a.dtype) for a in (*weights, *means, *variances)]
    return pl.pallas_call(
        functools.partial(adam_kernel, gathered),
        name="adamw_rest" if gathered else "adamw",
        grid=(count * CUT,),
        in_specs=mine * 3 + [spec(m) for m in range(3)] + ([pl.BlockSpec(memory_space=pl.ANY)] * 9 if gathered else []),
        out_specs=mine * 3,
        out_shape=shapes,
        input_output_aliases={12 + k: k for k in range(9)} if gathered else {},
        scratch_shapes=[pltpu.VMEM((rows, SL), BF)] if gathered else [],
        compiler_params=pltpu.CompilerParams(vmem_limit_bytes=VMEM_LIMIT),
        cost_estimate=pl.CostEstimate(flops=10**10, bytes_accessed=66 * D * SL * count, transcendentals=3 * D * SL * count),
    )(*weights, *means, *variances, *[gradients] * 3, *(so_far or ()))


def solution(mesh):
    def step(x, dy, *arrays):
        x, dy = x[0], dy[0]
        weights, means, variances = (arrays[k : k + 3] for k in (0, 3, 6))
        g1, g0 = gradients(x, dy, *weights)
        g0 = lax.all_gather(g0, "dp", axis=0)
        new = adam(0, NS + Q, weights, means, variances, g1)
        return tuple(adam(NS + Q, NS - Q, weights, means, variances, g0, new))

    return jax.shard_map(
        step,
        mesh=mesh,
        in_specs=(P(("rep", "dp"), None, None),) * 2 + (P(None, None, None),) * 9,
        out_specs=(P("rep", None, None),) * 9,
        check_vma=False,
    )
```

```python
import functools

import jax
import jax.numpy as jnp
from jax import lax
from jax.experimental import pallas as pl
from jax.experimental.pallas import tpu as pltpu
from jax.sharding import PartitionSpec as P

T, D, FF, SL = 2048, 1024, 3328, 256
NS = FF // SL
TB = 512
H = 256
FH = 512
PIECES = 8
F32, BF = jnp.float32, jnp.bfloat16
MESH = pl.DeviceIdType.MESH
VMEM_LIMIT = 66_900_000

STEPS1, MID, STEPS0 = 4, 4, 2
START0 = STEPS1 * NS + MID
OFF1 = (0, 2, 5, 7, 9, 11, 13, 15, 17, 20, 23, 26, 29)
OFF0 = (0, 2, 5, 7, 9, 11, 15, 17, 21, 24, 27, 30, 33)
NR = 12
SLOTS, SEMS, CB = 4, 4, 8
Q = 3
CUT = 1


def dot(a, b):
    return lax.dot_general(a, b, (((1,), (0,)), ((), ())), preferred_element_type=F32)


def dot_nt(a, b):
    return lax.dot_general(a, b, (((1,), (1,)), ((), ())), preferred_element_type=F32)


def normed(h):
    wide = h.astype(F32)
    scale = lax.rsqrt(jnp.mean(wide * wide, -1, keepdims=True) + 1e-6)
    return (wide * scale).astype(BF)


def pipelined(count, parts, *stages):
    size = T // count // parts

    def one(b, c):
        rows = [pl.ds(pl.multiple_of(b * (size * parts) + p * size, size), size) for p in range(parts)]
        values = [()] * parts
        for step in range(parts + len(stages) - 1):
            for k, stage in enumerate(stages):
                p = step - k
                if 0 <= p < parts:
                    out = stage(rows[p], *values[p])
                    values[p] = out if isinstance(out, tuple) else (out,)
        return c

    lax.fori_loop(0, count, one, 0)


def step_kernel(
    x_ref, dy_ref, wg_ref, wu_ref, wd_ref,
    g1_ref, g0_ref, gate_ref, up_ref, h1_ref, a0t_ref,
    act, by, actt, byt, acc, hid, dgt, dup, wgb, wub, wdb,
    grad, s1, s2, sa0, ra0, sb0, rb0, sa1, ra1, sb1, rb1, sa2, ra2, sb2, rb2, cb, g0b,
    wsem, asem, osem, xsem, lsem, send, recv,
):
    me = lax.axis_index("dp")
    xyz = (lax.div(me, 16), lax.rem(lax.div(me, 4), 4), lax.rem(me, 4))
    stride = (16, 4, 1)
    axes = [[(m + k) % 3 for k in range(3)] for m in range(3)]
    plus = [me + (lax.rem(xyz[d] + 1, 4) - xyz[d]) * stride[d] for d in range(3)]
    minus = [me + (lax.rem(xyz[d] + 3, 4) - xyz[d]) * stride[d] for d in range(3)]
    digit = [[xyz[d] for d in axes[m]] for m in range(3)]
    to = [[(plus[d], minus[d]) for d in axes[m]] for m in range(3)]

    def turn(c, k):
        return lax.rem(c + k, 4)

    def block(c, size):
        return pl.ds(pl.multiple_of(c * size, size), size)

    barrier = pltpu.get_barrier_semaphore()
    for d in range(3):
        for n in (plus[d], minus[d]):
            pl.semaphore_signal(barrier, inc=1, device_id={"dp": n}, device_id_type=MESH)

    HALF = (pl.ds(0, 128), pl.ds(128, 128))
    sas, ras, sbs, rbs = (sa0, sa1, sa2), (ra0, ra1, ra2), (sb0, sb1, sb2), (rb0, rb1, rb2)
    sizes = (256, 64, 16)

    def parts(r, s, m, k):
        slot = lax.rem(s, SLOTS)
        if r < 6:
            ph = r // 2
            send_buf, recv_buf = (sas[ph], ras[ph]) if r % 2 == 0 else (sbs[ph], rbs[ph])
            return send_buf.at[slot, m, k], recv_buf.at[slot, m, k]
        cbm = cb.at[lax.rem(s, CB), m]
        ph = 2 - (r - 6) // 2
        c = digit[m][ph]
        if r % 2 == 1:
            c = turn(c, 3 if k == 0 else 1)
        rows = block(digit[m][1] * 4 + c, 16) if ph == 2 else block(c, sizes[ph])
        if ph == 0:
            out = g1_ref.at[m, s, rows]
            return (cbm, out) if r % 2 == 0 else (out.at[:, HALF[k]], out.at[:, HALF[k]])
        at = cbm.at[rows] if r % 2 == 0 else cbm.at[rows, HALF[k]]
        return at, at

    def copies(r, s):
        slot = lax.rem(s, SEMS)
        ph = r // 2 if r < 6 else 2 - (r - 6) // 2
        for m in range(3):
            for k in range(2):
                src, dst = parts(r, s, m, k)
                yield pltpu.make_async_remote_copy(
                    src_ref=src,
                    dst_ref=dst,
                    send_sem=send.at[r, slot, m, k],
                    recv_sem=recv.at[r, slot, m, k],
                    device_id={"dp": to[m][ph][k]},
                    device_id_type=MESH,
                )

    def own_copy(s, m):
        return pltpu.make_async_copy(
            cb.at[lax.rem(s, CB), m], g1_ref.at[m, s, block(digit[m][0], 256)], lsem.at[lax.rem(s, SEMS), m]
        )

    def total(ph, s):
        return grad.at[pl.ds(pl.multiple_of(4 * lax.rem(s, 2), 4), 4)] if ph == 0 else (s1, s2)[ph - 1].at[lax.rem(s, SLOTS)]

    def mine(ph, s, m):
        slot = lax.rem(s, SLOTS)
        rows = block(digit[m][ph], sizes[ph])
        so_far = s1[slot, m] if ph == 0 else total(ph, s)[m, rows, :]
        return so_far + rbs[ph][slot, m, 0].astype(F32) + rbs[ph][slot, m, 1].astype(F32)

    def prepare(r, s):
        slot = lax.rem(s, SLOTS)
        if r > 0:
            for copy in copies(r - 1, s):
                copy.wait()
        for m in range(3):
            ph = r // 2
            if r in (2, 4):
                total(ph, s)[m] = mine(ph - 1, s, m)
            if r in (0, 2, 4):
                far = block(turn(digit[m][ph], 2), sizes[ph])
                for k in range(2):
                    sas[ph][slot, m, k] = total(ph, s)[m, far, HALF[k]].astype(BF)
            if r in (1, 3, 5):
                for k in range(2):
                    near = block(turn(digit[m][ph], 1 if k == 0 else 3), sizes[ph])
                    add, keep = HALF[k], HALF[1 - k]
                    sbs[ph][slot, m, k, :, add] = (total(ph, s)[m, near, add] + ras[ph][slot, m, k].astype(F32)).astype(BF)
                    sbs[ph][slot, m, k, :, keep] = total(ph, s)[m, near, keep].astype(BF)
            if r == 1:
                s1[slot, m] = total(0, s)[m, block(digit[m][0], 256), :]
            if r == 6:
                done = mine(2, s, m).astype(BF)

                @pl.when(s < NS + Q)
                def _():
                    cb[lax.rem(s, CB), m, block(digit[m][1] * 4 + digit[m][2], 16), :] = done

                @pl.when(s >= NS + Q)
                def _():
                    g0b[m, s - NS - Q] = done

            if r == NR:
                own_copy(s, m).wait()

    def start(r, s):
        for copy in copies(r, s):
            copy.start()
        if r == 10:
            for m in range(3):
                own_copy(s, m).start()

    def service(h):
        q1, r1 = lax.div(h, STEPS1), lax.rem(h, STEPS1)
        q0, r0 = lax.div(h, STEPS0), lax.rem(h, STEPS0)

        def some(parity):
            todo = []
            for r in (2, 3, 4, 5, 0, 1, 6, 7, 8, 9, 10, 11, 12):
                from1, from0 = STEPS1 - 1 + OFF1[r], START0 + STEPS0 - 1 + OFF0[r]
                if from1 % 2 != parity:
                    continue
                one = (r1 == from1 % STEPS1) & (h >= from1) & (h < from1 + STEPS1 * NS)

                def zero(count):
                    return (r0 == from0 % STEPS0) & (h >= from0) & (h < from0 + STEPS0 * count)

                s = jnp.where(h >= from0, NS + q0 - from0 // STEPS0, q1 - from1 // STEPS1)
                prepared = one | zero(NS if r <= 6 else Q)
                todo.append((r, s, prepared, one | zero(Q) if r == 6 else prepared))
            for r, s, prepared, _ in todo:
                if r <= 6:
                    pl.when(prepared)(functools.partial(prepare, r, s))
            for r, s, _, sent in todo:

                @pl.when(sent)
                def _():
                    if r > 6:
                        prepare(r, s)
                    if r < NR:
                        start(r, s)

        for parity in range(2):
            pl.when(lax.rem(h, 2) == parity)(functools.partial(some, parity))

    def weights(i):
        slot = lax.rem(i, 2)
        first = i < NS
        j = lax.rem(i, NS)
        columns = block(j, SL)
        down = pltpu.make_async_copy(wd_ref.at[jnp.where(first, 1, 0), columns, :], wdb.at[slot], wsem.at[slot, 0])
        one = [
            pltpu.make_async_copy(wg_ref.at[1, :, columns], wgb.at[slot], wsem.at[slot, 1]),
            pltpu.make_async_copy(wu_ref.at[1, :, columns], wub.at[slot], wsem.at[slot, 2]),
        ]
        zero = [
            pltpu.make_async_copy(gate_ref.at[j], acc.at[2 * slot], wsem.at[slot, 1]),
            pltpu.make_async_copy(up_ref.at[j], acc.at[2 * slot + 1], wsem.at[slot, 2]),
        ]
        return down, one, zero

    def first_weights(j):
        slot, columns = lax.rem(j, 2), block(j, SL)
        return [
            pltpu.make_async_copy(wg_ref.at[0, :, columns], wgb.at[slot], wsem.at[slot, 0]),
            pltpu.make_async_copy(wu_ref.at[0, :, columns], wub.at[slot], wsem.at[slot, 1]),
            pltpu.make_async_copy(wd_ref.at[0, columns, :], wdb.at[slot], wsem.at[slot, 2]),
        ]

    def kept(j):
        slot = lax.rem(j, 2)
        return [
            pltpu.make_async_copy(grad.at[4 * slot + 2 * k + half], ref.at[j, pl.ds(half * D, D)], osem.at[slot, k, half])
            for k, ref in enumerate((gate_ref, up_ref))
            for half in range(2)
        ]

    x_load = pltpu.make_async_copy(x_ref, act, asem.at[0])
    dy_load = pltpu.make_async_copy(dy_ref, by, asem.at[1])
    for copy in [x_load, *first_weights(0), dy_load]:
        copy.start()

    def clear(rows):
        for n in range(4):
            acc[n, rows, :] = jnp.zeros((TB, SL), F32)

    x_load.wait()

    columns = [ref.at[...] for ref in (hid, dgt, dup)]
    lasts = [sb0.at[b // 6, b % 6 // 2, b % 2] for b in range(T // H)]
    last_columns = pl.ds(3 * SL, SL)

    def moves(ref, out):
        pairs = [(part, ref.at[:, pl.ds(n * SL, SL)]) for n, part in enumerate(columns)]
        pairs += [(part, ref.at[pl.ds(b * H, H), last_columns]) for b, part in enumerate(lasts)]
        return [pltpu.make_async_copy(*(pair if out else pair[::-1]), xsem.at[n]) for n, pair in enumerate(pairs)]

    again = moves(x_ref, False)
    for copy in again:
        copy.start()

    def enter(b, c):
        rows = block(b, TB)
        act[rows, :] = normed(act[rows, :])
        clear(rows)
        return c

    lax.fori_loop(0, T // TB, enter, 0)
    dy_load.wait()

    def forward(j, c):
        slot = lax.rem(j, 2)
        for copy in first_weights(j):
            copy.wait()

        @pl.when(j + 1 < NS)
        def _():
            for copy in first_weights(j + 1):
                copy.start()

        @pl.when(j >= 2)
        def _():
            for copy in kept(j - 2):
                copy.wait()

        piece = block(jnp.minimum(j, PIECES - 1), T // PIECES)
        actt[:, piece] = act[piece, :].T
        byt[:, piece] = by[piece, :].T

        def gate_up(p):
            a = act[p * FH : p * FH + FH, :]
            return dot(a, wgb[slot]), dot(a, wub[slot])

        def hidden(p, gate, up):
            half, at = divmod(p * FH, D)
            grad[4 * slot + half, at : at + FH, :] = gate
            grad[4 * slot + 2 + half, at : at + FH, :] = up
            return ((gate * jax.nn.sigmoid(gate) * up).astype(BF),)

        def down(p, hidden):
            for n in range(4):
                acc[n, p * FH : p * FH + FH, :] += dot(hidden, wdb[slot, :, n * SL : n * SL + SL])

        parts = T // FH
        values = [()] * parts
        for at in range(parts + 2):
            for k, work in enumerate((gate_up, hidden, down)):
                if 0 <= at - k < parts:
                    values[at - k] = work(at - k, *values[at - k])
        for copy in kept(j):
            copy.start()
        return c

    lax.fori_loop(0, NS, forward, 0)
    a0t_keep = pltpu.make_async_copy(actt, a0t_ref, asem.at[2])
    a0t_keep.start()
    down, one, _ = weights(0)
    for copy in [down, *one]:
        copy.start()
    for copy in [*kept(NS - 2), *kept(NS - 1), *again]:
        copy.wait()
    for b in range(T // H):
        rows = pl.ds(b * H, H)
        pieces = [part.at[rows] for part in columns] + [lasts[b]]
        h1 = []
        for n, part in enumerate(pieces):
            h1.append((part[...].astype(F32) + acc[n, rows, :].astype(BF).astype(F32)).astype(BF))
            part[...] = h1[n]
            acc[n, rows, :] = jnp.zeros((H, SL), F32)
        act[rows, :] = normed(jnp.concatenate(h1, axis=1))
    a0t_keep.wait()
    keep = moves(h1_ref, True)
    for copy in keep:
        copy.start()

    def turned(b, c):
        rows = block(b, H)
        actt[:, rows] = act[rows, :].T
        return c

    lax.fori_loop(0, T // H, turned, 0)
    for copy in keep:
        copy.wait()
    pl.semaphore_wait(barrier, 6)
    h1_load = pltpu.make_async_copy(h1_ref, act, asem.at[0])
    a0t_load = pltpu.make_async_copy(a0t_ref, actt, asem.at[2])

    def second_layer(i, part):
        slot = lax.rem(i, 2)

        @pl.when(part == 0)
        def _():
            down, one, _ = weights(i)
            for copy in [down, *one]:
                copy.wait()

            @pl.when(i + 1 < NS)
            def _():
                down, one, _ = weights(i + 1)
                for copy in [down, *one]:
                    copy.start()

        def products(rows):
            a = act[rows, :]
            return dot(a, wgb[slot]), dot(a, wub[slot]), dot_nt(by[rows, :], wdb[slot])

        def elements(rows, gate, up, by_hid):
            by_hid = by_hid.astype(BF).astype(F32)
            sig = jax.nn.sigmoid(gate)
            silu = gate * sig
            hid[rows, :] = (silu * up).astype(BF)
            by_up = (by_hid * silu).astype(BF)
            by_gate = (by_hid * up * (sig * (1.0 + gate * (1.0 - sig)))).astype(BF)
            dup[rows, :] = by_up
            dgt[rows, :] = by_gate
            return by_gate, by_up

        def back(rows, by_gate, by_up):
            for n in range(4):
                acc[n, rows, :] += dot_nt(by_gate, wgb[slot, pl.ds(n * SL, SL), :]) + dot_nt(by_up, wub[slot, pl.ds(n * SL, SL), :])

        half = T // 2
        count = half // H
        rows = [pl.ds(pl.multiple_of(part * half + p * H, H), H) for p in range(count)]
        d, e = [None] * count, [None] * count
        for p in range(count + 2):
            if p < count:
                d[p] = products(rows[p])
            if 0 <= p - 1 < count:
                e[p - 1] = elements(rows[p - 1], *d[p - 1])
            if 0 <= p - 2 < count:
                back(rows[p - 2], *e[p - 2])

    def between(part):
        @pl.when(part == 0)
        def _():
            h1_load.wait()
            a0t_load.start()
            weights(NS)[0].start()

        quarter = T // MID

        def tokens(b, c):
            rows = pl.ds(pl.multiple_of(part * quarter + b * H, H), H)
            wide = act[rows, :].astype(F32)
            scale = lax.rsqrt(jnp.mean(wide * wide, -1, keepdims=True) + 1e-6)
            da = jnp.concatenate([acc[n, rows, :] for n in range(4)], axis=1).astype(BF).astype(F32)
            t = jnp.mean(da * wide, -1, keepdims=True)
            dwide = (da * scale - wide * (scale * scale * scale * t)).astype(BF)
            by_h = (by[rows, :].astype(F32) + dwide.astype(F32)).astype(BF)
            by[rows, :] = by_h
            byt[:, rows] = by_h.T
            return c

        lax.fori_loop(0, quarter // H, tokens, 0)

        @pl.when(part == MID - 1)
        def _():
            for copy in weights(NS)[2]:
                copy.start()
            a0t_load.wait()

    def first_layer(i):
        slot = lax.rem(i, 2)
        down, _, zero = weights(i)
        for copy in [down, *zero]:
            copy.wait()

        @pl.when(i + 1 < 2 * NS)
        def _():
            down, _, zero = weights(i + 1)
            for copy in [down, *zero]:
                copy.start()

        def products(rows):
            return dot_nt(by[rows, :], wdb[slot])

        def elements(rows, by_hid):
            gate = acc[2 * slot, rows, :]
            up = acc[2 * slot + 1, rows, :]
            by_hid = by_hid.astype(BF).astype(F32)
            sig = jax.nn.sigmoid(gate)
            silu = gate * sig
            hid[rows, :] = (silu * up).astype(BF)
            dup[rows, :] = (by_hid * silu).astype(BF)
            dgt[rows, :] = (by_hid * up * (sig * (1.0 + gate * (1.0 - sig)))).astype(BF)

        pipelined(T // TB, TB // H, products, elements)

    def gradient(s, m):
        left, right = ((actt, dgt), (actt, dup), (byt, hid))[m]
        grad[4 * lax.rem(s, 2) + m] = dot(left[...], right[...])

    def step(h, c):
        in1 = h < STEPS1 * NS
        in0 = (h >= START0) & (h < START0 + STEPS0 * NS)
        h0 = h - START0
        s = jnp.where(in1, lax.div(h, STEPS1), NS + lax.div(h0, STEPS0))
        part = jnp.where(in1, lax.rem(h, STEPS1), lax.rem(h0, STEPS0))

        @pl.when(in1)
        def _():
            @pl.when(part < 2)
            def _():
                second_layer(s, part)

            @pl.when(h == STEPS1 * NS - 1)
            def _():
                h1_load.start()

        @pl.when(h >= STEPS1 * NS)
        def _():
            @pl.when(h < START0)
            def _():
                between(h - STEPS1 * NS)

            @pl.when(in0 & (part == 0))
            def _():
                first_layer(s)

        @pl.when((in1 & (part == STEPS1 - 2)) | (in0 & (part == 0)))
        def _():
            gradient(s, 0)

        @pl.when((in1 & (part == STEPS1 - 1)) | (in0 & (part == 1)))
        def _():
            gradient(s, 1)
            gradient(s, 2)

        service(h)
        return c

    last = max(START0 + STEPS0 * NS + OFF0[6], STEPS1 * NS + OFF1[NR], START0 + STEPS0 * Q + OFF0[NR])
    lax.fori_loop(0, last, step, 0)
    out = pltpu.make_async_copy(g0b, g0_ref, asem.at[0])
    out.start()
    out.wait()


def gradients(x, dy, wg, wu, wd):
    anyspec = pl.BlockSpec(memory_space=pl.ANY)
    V = pltpu.VMEM
    DMA = pltpu.SemaphoreType.DMA
    return pl.pallas_call(
        step_kernel,
        name="gradients",
        in_specs=[anyspec] * 5,
        out_specs=[anyspec] * 6,
        out_shape=[
            jax.ShapeDtypeStruct((3, NS + Q, D, SL), BF),
            jax.ShapeDtypeStruct((3, NS - Q, 16, SL), BF),
            jax.ShapeDtypeStruct((NS, T, SL), F32),
            jax.ShapeDtypeStruct((NS, T, SL), F32),
            jax.ShapeDtypeStruct((T, D), BF),
            jax.ShapeDtypeStruct((D, T), BF),
        ],
        scratch_shapes=[
            V((T, D), BF), V((T, D), BF), V((D, T), BF), V((D, T), BF), V((4, T, SL), F32),
            V((T, SL), BF), V((T, SL), BF), V((T, SL), BF),
            V((2, D, SL), BF), V((2, D, SL), BF), V((2, SL, D), BF),
            V((8, D, SL), F32), V((SLOTS, 3, 256, SL), F32), V((SLOTS, 3, 64, SL), F32),
            *[V((SLOTS, 3, 2, size, width), BF) for size in (256, 64, 16) for width in (128, 128, SL, SL)],
            V((CB, 3, 256, SL), BF), V((3, NS - Q, 16, SL), BF),
            DMA((2, 3)), DMA((4,)), DMA((2, 2, 2)), DMA((11,)), DMA((SEMS, 3)), DMA((NR, SEMS, 3, 2)), DMA((NR, SEMS, 3, 2)),
        ],
        compiler_params=pltpu.CompilerParams(vmem_limit_bytes=VMEM_LIMIT, collective_id=0, has_side_effects=True),
        cost_estimate=pl.CostEstimate(flops=30 * T * D * FF, bytes_accessed=250_000_000, transcendentals=3 * T * FF),
    )(x, dy, wg, wu, wd)[:2]


def adam_kernel(gathered, *refs):
    ins, rest = refs[:12], refs[12:]
    if gathered:
        rest = rest[9:]
    outs, rest = rest[:9], rest[9:]
    for m in range(3):
        w_ref, m_ref, v_ref, g_ref = ins[m], ins[3 + m], ins[6 + m], ins[9 + m]
        w_out, m_out, v_out = outs[m], outs[3 + m], outs[6 + m]

        def take(at, g):
            g = g.astype(F32)
            w = w_ref[at].astype(F32)
            mean = 0.9 * m_ref[at] + 0.1 * g
            var = 0.95 * v_ref[at] + 0.05 * g * g
            w_out[at] = (w - 0.02 * (mean * lax.rsqrt(var + 1e-8) + 0.1 * w)).astype(BF)
            m_out[at] = mean
            v_out[at] = var

        if gathered:
            whole = rest[0]
            for n in range(64 // CUT):
                digits = (n // 16, n // 4 % 4, n % 4)
                x, y, z = (digits[(d - m) % 3] for d in range(3))
                whole[n * 16 : n * 16 + 16, :] = g_ref[x, y, z, 0, 0]
            look = lambda rows: whole[rows, :]
        else:
            look = lambda rows: g_ref[0, 0, rows, :]

        if m < 2:

            def one(b, c):
                rows = pl.ds(pl.multiple_of(b * 64, 64), 64)
                take((0, rows, slice(None)), look(rows))
                return c

            lax.fori_loop(0, D // CUT // 64, one, 0)
        else:

            def one(b, c):
                rows = pl.ds(pl.multiple_of(b * 128, 128), 128)
                take((0, slice(None), rows), look(rows).T)
                return c

            lax.fori_loop(0, D // CUT // 128, one, 0)


def adam(first, count, weights, means, variances, gradients, so_far=None):
    rows = D // CUT

    def place(j):
        s = first + j // CUT
        return jnp.where(s < NS, 1, 0), jnp.where(s < NS, s, s - NS), j % CUT

    def at_wide(j):
        layer, column, row = place(j)
        return layer, row, column

    wide = pl.BlockSpec((1, rows, SL), at_wide)
    tall = pl.BlockSpec((1, SL, rows), place)
    mine = [wide, wide, tall]
    gathered = so_far is not None
    if gathered:
        gradients = gradients.reshape(4, 4, 4, *gradients.shape[1:])

        def spec(m):
            return pl.BlockSpec(
                tuple(4 // CUT if d == m else 4 for d in range(3)) + (1, 1, 16, SL),
                lambda j: tuple(j % CUT if d == m else 0 for d in range(3)) + (m, j // CUT, 0, 0),
            )

    else:

        def spec(m):
            return pl.BlockSpec((1, 1, rows, SL), lambda j: (m, j // CUT, j % CUT, 0))

    shapes = [jax.ShapeDtypeStruct(a.shape, a.dtype) for a in (*weights, *means, *variances)]
    return pl.pallas_call(
        functools.partial(adam_kernel, gathered),
        name="adamw_rest" if gathered else "adamw",
        grid=(count * CUT,),
        in_specs=mine * 3 + [spec(m) for m in range(3)] + ([pl.BlockSpec(memory_space=pl.ANY)] * 9 if gathered else []),
        out_specs=mine * 3,
        out_shape=shapes,
        input_output_aliases={12 + k: k for k in range(9)} if gathered else {},
        scratch_shapes=[pltpu.VMEM((rows, SL), BF)] if gathered else [],
        compiler_params=pltpu.CompilerParams(vmem_limit_bytes=VMEM_LIMIT),
        cost_estimate=pl.CostEstimate(flops=10**10, bytes_accessed=66 * D * SL * count, transcendentals=3 * D * SL * count),
    )(*weights, *means, *variances, *[gradients] * 3, *(so_far or ()))


def solution(mesh):
    def step(x, dy, *arrays):
        x, dy = x[0], dy[0]
        weights, means, variances = (arrays[k : k + 3] for k in (0, 3, 6))
        g1, g0 = gradients(x, dy, *weights)
        g0 = lax.all_gather(g0, "dp", axis=0)
        new = adam(0, NS + Q, weights, means, variances, g1)
        return tuple(adam(NS + Q, NS - Q, weights, means, variances, g0, new))

    return jax.shard_map(
        step,
        mesh=mesh,
        in_specs=(P(("rep", "dp"), None, None),) * 2 + (P(None, None, None),) * 9,
        out_specs=(P("rep", None, None),) * 9,
        check_vma=False,
    )
```

```python
import functools

import jax
import jax.numpy as jnp
from jax import lax
from jax.experimental import pallas as pl
from jax.experimental.pallas import tpu as pltpu
from jax.sharding import PartitionSpec as P

T, D, FF, SL = 2048, 1024, 3328, 256
NS = FF // SL
TB = 512
H = 256
FH = 512
PIECES = 8
F32, BF = jnp.float32, jnp.bfloat16
MESH = pl.DeviceIdType.MESH
VMEM_LIMIT = 66_900_000

STEPS1, MID, STEPS0 = 4, 4, 2
START0 = STEPS1 * NS + MID
OFF1 = (0, 2, 5, 7, 9, 11, 13, 15, 17, 20, 23, 26, 29)
OFF0 = (0, 2, 5, 7, 9, 11, 15, 17, 21, 24, 27, 30, 33)
NR = 12
SLOTS, SEMS, CB = 4, 4, 8
Q = 3
CUT = 1


def dot(a, b):
    return lax.dot_general(a, b, (((1,), (0,)), ((), ())), preferred_element_type=F32)


def dot_nt(a, b):
    return lax.dot_general(a, b, (((1,), (1,)), ((), ())), preferred_element_type=F32)


def normed(h):
    wide = h.astype(F32)
    scale = lax.rsqrt(jnp.mean(wide * wide, -1, keepdims=True) + 1e-6)
    return (wide * scale).astype(BF)


def pipelined(count, parts, *stages):
    size = T // count // parts

    def one(b, c):
        rows = [pl.ds(pl.multiple_of(b * (size * parts) + p * size, size), size) for p in range(parts)]
        values = [()] * parts
        for step in range(parts + len(stages) - 1):
            for k, stage in enumerate(stages):
                p = step - k
                if 0 <= p < parts:
                    out = stage(rows[p], *values[p])
                    values[p] = out if isinstance(out, tuple) else (out,)
        return c

    lax.fori_loop(0, count, one, 0)


def step_kernel(
    x_ref, dy_ref, wg_ref, wu_ref, wd_ref,
    g1_ref, g0_ref, gate_ref, up_ref, h1_ref, a0t_ref,
    act, by, actt, byt, acc, hid, dgt, dup, wgb, wub, wdb,
    grad, s1, s2, sa0, ra0, sb0, rb0, sa1, ra1, sb1, rb1, sa2, ra2, sb2, rb2, cb, g0b,
    wsem, asem, osem, xsem, lsem, send, recv,
):
    me = lax.axis_index("dp")
    xyz = (lax.div(me, 16), lax.rem(lax.div(me, 4), 4), lax.rem(me, 4))
    stride = (16, 4, 1)
    axes = [[(m + k) % 3 for k in range(3)] for m in range(3)]
    plus = [me + (lax.rem(xyz[d] + 1, 4) - xyz[d]) * stride[d] for d in range(3)]
    minus = [me + (lax.rem(xyz[d] + 3, 4) - xyz[d]) * stride[d] for d in range(3)]
    digit = [[xyz[d] for d in axes[m]] for m in range(3)]
    to = [[(plus[d], minus[d]) for d in axes[m]] for m in range(3)]

    def turn(c, k):
        return lax.rem(c + k, 4)

    def block(c, size):
        return pl.ds(pl.multiple_of(c * size, size), size)

    barrier = pltpu.get_barrier_semaphore()
    for d in range(3):
        for n in (plus[d], minus[d]):
            pl.semaphore_signal(barrier, inc=1, device_id={"dp": n}, device_id_type=MESH)

    HALF = (pl.ds(0, 128), pl.ds(128, 128))
    sas, ras, sbs, rbs = (sa0, sa1, sa2), (ra0, ra1, ra2), (sb0, sb1, sb2), (rb0, rb1, rb2)
    sizes = (256, 64, 16)

    def parts(r, s, m, k):
        slot = lax.rem(s, SLOTS)
        if r < 6:
            ph = r // 2
            send_buf, recv_buf = (sas[ph], ras[ph]) if r % 2 == 0 else (sbs[ph], rbs[ph])
            return send_buf.at[slot, m, k], recv_buf.at[slot, m, k]
        cbm = cb.at[lax.rem(s, CB), m]
        ph = 2 - (r - 6) // 2
        c = digit[m][ph]
        if r % 2 == 1:
            c = turn(c, 3 if k == 0 else 1)
        rows = block(digit[m][1] * 4 + c, 16) if ph == 2 else block(c, sizes[ph])
        if ph == 0:
            out = g1_ref.at[m, s, rows]
            return (cbm, out) if r % 2 == 0 else (out.at[:, HALF[k]], out.at[:, HALF[k]])
        at = cbm.at[rows] if r % 2 == 0 else cbm.at[rows, HALF[k]]
        return at, at

    def copies(r, s):
        slot = lax.rem(s, SEMS)
        ph = r // 2 if r < 6 else 2 - (r - 6) // 2
        for m in range(3):
            for k in range(2):
                src, dst = parts(r, s, m, k)
                yield pltpu.make_async_remote_copy(
                    src_ref=src,
                    dst_ref=dst,
                    send_sem=send.at[r, slot, m, k],
                    recv_sem=recv.at[r, slot, m, k],
                    device_id={"dp": to[m][ph][k]},
                    device_id_type=MESH,
                )

    def own_copy(s, m):
        return pltpu.make_async_copy(
            cb.at[lax.rem(s, CB), m], g1_ref.at[m, s, block(digit[m][0], 256)], lsem.at[lax.rem(s, SEMS), m]
        )

    def total(ph, s):
        return grad.at[pl.ds(pl.multiple_of(4 * lax.rem(s, 2), 4), 4)] if ph == 0 else (s1, s2)[ph - 1].at[lax.rem(s, SLOTS)]

    def mine(ph, s, m):
        slot = lax.rem(s, SLOTS)
        rows = block(digit[m][ph], sizes[ph])
        so_far = s1[slot, m] if ph == 0 else total(ph, s)[m, rows, :]
        return so_far + rbs[ph][slot, m, 0].astype(F32) + rbs[ph][slot, m, 1].astype(F32)

    def prepare(r, s):
        slot = lax.rem(s, SLOTS)
        if r > 0:
            for copy in copies(r - 1, s):
                copy.wait()
        for m in range(3):
            ph = r // 2
            if r in (2, 4):
                total(ph, s)[m] = mine(ph - 1, s, m)
            if r in (0, 2, 4):
                far = block(turn(digit[m][ph], 2), sizes[ph])
                for k in range(2):
                    sas[ph][slot, m, k] = total(ph, s)[m, far, HALF[k]].astype(BF)
            if r in (1, 3, 5):
                for k in range(2):
                    near = block(turn(digit[m][ph], 1 if k == 0 else 3), sizes[ph])
                    add, keep = HALF[k], HALF[1 - k]
                    sbs[ph][slot, m, k, :, add] = (total(ph, s)[m, near, add] + ras[ph][slot, m, k].astype(F32)).astype(BF)
                    sbs[ph][slot, m, k, :, keep] = total(ph, s)[m, near, keep].astype(BF)
            if r == 1:
                s1[slot, m] = total(0, s)[m, block(digit[m][0], 256), :]
            if r == 6:
                done = mine(2, s, m).astype(BF)

                @pl.when(s < NS + Q)
                def _():
                    cb[lax.rem(s, CB), m, block(digit[m][1] * 4 + digit[m][2], 16), :] = done

                @pl.when(s >= NS + Q)
                def _():
                    g0b[m, s - NS - Q] = done

            if r == NR:
                own_copy(s, m).wait()

    def start(r, s):
        for copy in copies(r, s):
            copy.start()
        if r == 10:
            for m in range(3):
                own_copy(s, m).start()

    def service(h):
        q1, r1 = lax.div(h, STEPS1), lax.rem(h, STEPS1)
        q0, r0 = lax.div(h, STEPS0), lax.rem(h, STEPS0)

        def some(alone, kind):
            todo = []
            for r in (2, 3, 4, 5, 0, 1, 6, 7, 8, 9, 10, 11, 12):
                from1, from0 = STEPS1 - 1 + OFF1[r], START0 + STEPS0 - 1 + OFF0[r]
                if from1 % (STEPS1 if alone else 2) != kind:
                    continue
                one = (h >= from1) & (h < from1 + STEPS1 * NS)
                s = q1 - from1 // STEPS1
                if alone:
                    todo.append((r, s, one, one))
                    continue
                one = one & (r1 == from1 % STEPS1)

                def zero(count):
                    return (r0 == from0 % STEPS0) & (h >= from0) & (h < from0 + STEPS0 * count)

                s = jnp.where(h >= from0, NS + q0 - from0 // STEPS0, s)
                prepared = one | zero(NS if r <= 6 else Q)
                todo.append((r, s, prepared, one | zero(Q) if r == 6 else prepared))
            for r, s, prepared, _ in todo:
                if r <= 6:
                    pl.when(prepared)(functools.partial(prepare, r, s))
            for r, s, _, sent in todo:

                @pl.when(sent)
                def _():
                    if r > 6:
                        prepare(r, s)
                    if r < NR:
                        start(r, s)

        first = START0 + STEPS0 - 1

        @pl.when(h < first)
        def _():
            for kind in range(STEPS1):
                pl.when(r1 == kind)(functools.partial(some, True, kind))

        @pl.when(h >= first)
        def _():
            for kind in range(2):
                pl.when(lax.rem(h, 2) == kind)(functools.partial(some, False, kind))

    def weights(i):
        slot = lax.rem(i, 2)
        first = i < NS
        j = lax.rem(i, NS)
        columns = block(j, SL)
        down = pltpu.make_async_copy(wd_ref.at[jnp.where(first, 1, 0), columns, :], wdb.at[slot], wsem.at[slot, 0])
        one = [
            pltpu.make_async_copy(wg_ref.at[1, :, columns], wgb.at[slot], wsem.at[slot, 1]),
            pltpu.make_async_copy(wu_ref.at[1, :, columns], wub.at[slot], wsem.at[slot, 2]),
        ]
        zero = [
            pltpu.make_async_copy(gate_ref.at[j], acc.at[2 * slot], wsem.at[slot, 1]),
            pltpu.make_async_copy(up_ref.at[j], acc.at[2 * slot + 1], wsem.at[slot, 2]),
        ]
        return down, one, zero

    def first_weights(j):
        slot, columns = lax.rem(j, 2), block(j, SL)
        return [
            pltpu.make_async_copy(wg_ref.at[0, :, columns], wgb.at[slot], wsem.at[slot, 0]),
            pltpu.make_async_copy(wu_ref.at[0, :, columns], wub.at[slot], wsem.at[slot, 1]),
            pltpu.make_async_copy(wd_ref.at[0, columns, :], wdb.at[slot], wsem.at[slot, 2]),
        ]

    def kept(j):
        slot = lax.rem(j, 2)
        return [
            pltpu.make_async_copy(grad.at[4 * slot + 2 * k + half], ref.at[j, pl.ds(half * D, D)], osem.at[slot, k, half])
            for k, ref in enumerate((gate_ref, up_ref))
            for half in range(2)
        ]

    x_load = pltpu.make_async_copy(x_ref, act, asem.at[0])
    dy_load = pltpu.make_async_copy(dy_ref, by, asem.at[1])
    for copy in [x_load, *first_weights(0), dy_load]:
        copy.start()

    def clear(rows):
        for n in range(4):
            acc[n, rows, :] = jnp.zeros((TB, SL), F32)

    x_load.wait()

    columns = [ref.at[...] for ref in (hid, dgt, dup)]
    lasts = [sb0.at[b // 6, b % 6 // 2, b % 2] for b in range(T // H)]
    last_columns = pl.ds(3 * SL, SL)

    def moves(ref, out):
        pairs = [(part, ref.at[:, pl.ds(n * SL, SL)]) for n, part in enumerate(columns)]
        pairs += [(part, ref.at[pl.ds(b * H, H), last_columns]) for b, part in enumerate(lasts)]
        return [pltpu.make_async_copy(*(pair if out else pair[::-1]), xsem.at[n]) for n, pair in enumerate(pairs)]

    again = moves(x_ref, False)
    for copy in again:
        copy.start()

    def enter(b, c):
        rows = block(b, TB)
        act[rows, :] = normed(act[rows, :])
        clear(rows)
        return c

    lax.fori_loop(0, T // TB, enter, 0)
    dy_load.wait()

    def forward(j, c):
        slot = lax.rem(j, 2)
        for copy in first_weights(j):
            copy.wait()

        @pl.when(j + 1 < NS)
        def _():
            for copy in first_weights(j + 1):
                copy.start()

        @pl.when(j >= 2)
        def _():
            for copy in kept(j - 2):
                copy.wait()

        piece = block(jnp.minimum(j, PIECES - 1), T // PIECES)
        actt[:, piece] = act[piece, :].T
        byt[:, piece] = by[piece, :].T

        def gate_up(p):
            a = act[p * FH : p * FH + FH, :]
            return dot(a, wgb[slot]), dot(a, wub[slot])

        def hidden(p, gate, up):
            half, at = divmod(p * FH, D)
            grad[4 * slot + half, at : at + FH, :] = gate
            grad[4 * slot + 2 + half, at : at + FH, :] = up
            return ((gate * jax.nn.sigmoid(gate) * up).astype(BF),)

        def down(p, hidden):
            for n in range(4):
                acc[n, p * FH : p * FH + FH, :] += dot(hidden, wdb[slot, :, n * SL : n * SL + SL])

        parts = T // FH
        values = [()] * parts
        for at in range(parts + 2):
            for k, work in enumerate((gate_up, hidden, down)):
                if 0 <= at - k < parts:
                    values[at - k] = work(at - k, *values[at - k])
        for copy in kept(j):
            copy.start()
        return c

    lax.fori_loop(0, NS, forward, 0)
    a0t_keep = pltpu.make_async_copy(actt, a0t_ref, asem.at[2])
    a0t_keep.start()
    down, one, _ = weights(0)
    for copy in [down, *one]:
        copy.start()
    for copy in [*kept(NS - 2), *kept(NS - 1), *again]:
        copy.wait()
    for b in range(T // H):
        rows = pl.ds(b * H, H)
        pieces = [part.at[rows] for part in columns] + [lasts[b]]
        h1 = []
        for n, part in enumerate(pieces):
            h1.append((part[...].astype(F32) + acc[n, rows, :].astype(BF).astype(F32)).astype(BF))
            part[...] = h1[n]
            acc[n, rows, :] = jnp.zeros((H, SL), F32)
        act[rows, :] = normed(jnp.concatenate(h1, axis=1))
    a0t_keep.wait()
    keep = moves(h1_ref, True)
    for copy in keep:
        copy.start()

    def turned(b, c):
        rows = block(b, H)
        actt[:, rows] = act[rows, :].T
        return c

    lax.fori_loop(0, T // H, turned, 0)
    for copy in keep:
        copy.wait()
    pl.semaphore_wait(barrier, 6)
    h1_load = pltpu.make_async_copy(h1_ref, act, asem.at[0])
    a0t_load = pltpu.make_async_copy(a0t_ref, actt, asem.at[2])

    def second_layer(i, part):
        slot = lax.rem(i, 2)

        @pl.when(part == 0)
        def _():
            down, one, _ = weights(i)
            for copy in [down, *one]:
                copy.wait()

            @pl.when(i + 1 < NS)
            def _():
                down, one, _ = weights(i + 1)
                for copy in [down, *one]:
                    copy.start()

        def products(rows):
            a = act[rows, :]
            return dot(a, wgb[slot]), dot(a, wub[slot]), dot_nt(by[rows, :], wdb[slot])

        def elements(rows, gate, up, by_hid):
            by_hid = by_hid.astype(BF).astype(F32)
            sig = jax.nn.sigmoid(gate)
            silu = gate * sig
            hid[rows, :] = (silu * up).astype(BF)
            by_up = (by_hid * silu).astype(BF)
            by_gate = (by_hid * up * (sig * (1.0 + gate * (1.0 - sig)))).astype(BF)
            dup[rows, :] = by_up
            dgt[rows, :] = by_gate
            return by_gate, by_up

        def back(rows, by_gate, by_up):
            for n in range(4):
                acc[n, rows, :] += dot_nt(by_gate, wgb[slot, pl.ds(n * SL, SL), :]) + dot_nt(by_up, wub[slot, pl.ds(n * SL, SL), :])

        half = T // 2
        count = half // H
        rows = [pl.ds(pl.multiple_of(part * half + p * H, H), H) for p in range(count)]
        d, e = [None] * count, [None] * count
        for p in range(count + 2):
            if p < count:
                d[p] = products(rows[p])
            if 0 <= p - 1 < count:
                e[p - 1] = elements(rows[p - 1], *d[p - 1])
            if 0 <= p - 2 < count:
                back(rows[p - 2], *e[p - 2])

    def between(part):
        @pl.when(part == 0)
        def _():
            h1_load.wait()
            a0t_load.start()
            weights(NS)[0].start()

        quarter = T // MID

        def tokens(b, c):
            rows = pl.ds(pl.multiple_of(part * quarter + b * H, H), H)
            wide = act[rows, :].astype(F32)
            scale = lax.rsqrt(jnp.mean(wide * wide, -1, keepdims=True) + 1e-6)
            da = jnp.concatenate([acc[n, rows, :] for n in range(4)], axis=1).astype(BF).astype(F32)
            t = jnp.mean(da * wide, -1, keepdims=True)
            dwide = (da * scale - wide * (scale * scale * scale * t)).astype(BF)
            by_h = (by[rows, :].astype(F32) + dwide.astype(F32)).astype(BF)
            by[rows, :] = by_h
            byt[:, rows] = by_h.T
            return c

        lax.fori_loop(0, quarter // H, tokens, 0)

        @pl.when(part == MID - 1)
        def _():
            for copy in weights(NS)[2]:
                copy.start()
            a0t_load.wait()

    def first_layer(i):
        slot = lax.rem(i, 2)
        down, _, zero = weights(i)
        for copy in [down, *zero]:
            copy.wait()

        @pl.when(i + 1 < 2 * NS)
        def _():
            down, _, zero = weights(i + 1)
            for copy in [down, *zero]:
                copy.start()

        def products(rows):
            return dot_nt(by[rows, :], wdb[slot])

        def elements(rows, by_hid):
            gate = acc[2 * slot, rows, :]
            up = acc[2 * slot + 1, rows, :]
            by_hid = by_hid.astype(BF).astype(F32)
            sig = jax.nn.sigmoid(gate)
            silu = gate * sig
            hid[rows, :] = (silu * up).astype(BF)
            dup[rows, :] = (by_hid * silu).astype(BF)
            dgt[rows, :] = (by_hid * up * (sig * (1.0 + gate * (1.0 - sig)))).astype(BF)

        pipelined(T // TB, TB // H, products, elements)

    def gradient(s, m):
        left, right = ((actt, dgt), (actt, dup), (byt, hid))[m]
        grad[4 * lax.rem(s, 2) + m] = dot(left[...], right[...])

    def step(h, c):
        in1 = h < STEPS1 * NS
        in0 = (h >= START0) & (h < START0 + STEPS0 * NS)
        h0 = h - START0
        s = jnp.where(in1, lax.div(h, STEPS1), NS + lax.div(h0, STEPS0))
        part = jnp.where(in1, lax.rem(h, STEPS1), lax.rem(h0, STEPS0))

        @pl.when(in1)
        def _():
            @pl.when(part < 2)
            def _():
                second_layer(s, part)

            @pl.when(h == STEPS1 * NS - 1)
            def _():
                h1_load.start()

        @pl.when(h >= STEPS1 * NS)
        def _():
            @pl.when(h < START0)
            def _():
                between(h - STEPS1 * NS)

            @pl.when(in0 & (part == 0))
            def _():
                first_layer(s)

        @pl.when((in1 & (part == STEPS1 - 2)) | (in0 & (part == 0)))
        def _():
            gradient(s, 0)

        @pl.when((in1 & (part == STEPS1 - 1)) | (in0 & (part == 1)))
        def _():
            gradient(s, 1)
            gradient(s, 2)

        service(h)
        return c

    last = max(START0 + STEPS0 * NS + OFF0[6], STEPS1 * NS + OFF1[NR], START0 + STEPS0 * Q + OFF0[NR])
    lax.fori_loop(0, last, step, 0)
    out = pltpu.make_async_copy(g0b, g0_ref, asem.at[0])
    out.start()
    out.wait()


def gradients(x, dy, wg, wu, wd):
    anyspec = pl.BlockSpec(memory_space=pl.ANY)
    V = pltpu.VMEM
    DMA = pltpu.SemaphoreType.DMA
    return pl.pallas_call(
        step_kernel,
        name="gradients",
        in_specs=[anyspec] * 5,
        out_specs=[anyspec] * 6,
        out_shape=[
            jax.ShapeDtypeStruct((3, NS + Q, D, SL), BF),
            jax.ShapeDtypeStruct((3, NS - Q, 16, SL), BF),
            jax.ShapeDtypeStruct((NS, T, SL), F32),
            jax.ShapeDtypeStruct((NS, T, SL), F32),
            jax.ShapeDtypeStruct((T, D), BF),
            jax.ShapeDtypeStruct((D, T), BF),
        ],
        scratch_shapes=[
            V((T, D), BF), V((T, D), BF), V((D, T), BF), V((D, T), BF), V((4, T, SL), F32),
            V((T, SL), BF), V((T, SL), BF), V((T, SL), BF),
            V((2, D, SL), BF), V((2, D, SL), BF), V((2, SL, D), BF),
            V((8, D, SL), F32), V((SLOTS, 3, 256, SL), F32), V((SLOTS, 3, 64, SL), F32),
            *[V((SLOTS, 3, 2, size, width), BF) for size in (256, 64, 16) for width in (128, 128, SL, SL)],
            V((CB, 3, 256, SL), BF), V((3, NS - Q, 16, SL), BF),
            DMA((2, 3)), DMA((4,)), DMA((2, 2, 2)), DMA((11,)), DMA((SEMS, 3)), DMA((NR, SEMS, 3, 2)), DMA((NR, SEMS, 3, 2)),
        ],
        compiler_params=pltpu.CompilerParams(vmem_limit_bytes=VMEM_LIMIT, collective_id=0, has_side_effects=True),
        cost_estimate=pl.CostEstimate(flops=30 * T * D * FF, bytes_accessed=250_000_000, transcendentals=3 * T * FF),
    )(x, dy, wg, wu, wd)[:2]


def adam_kernel(gathered, *refs):
    ins, rest = refs[:12], refs[12:]
    if gathered:
        rest = rest[9:]
    outs, rest = rest[:9], rest[9:]
    for m in range(3):
        w_ref, m_ref, v_ref, g_ref = ins[m], ins[3 + m], ins[6 + m], ins[9 + m]
        w_out, m_out, v_out = outs[m], outs[3 + m], outs[6 + m]

        def take(at, g):
            g = g.astype(F32)
            w = w_ref[at].astype(F32)
            mean = 0.9 * m_ref[at] + 0.1 * g
            var = 0.95 * v_ref[at] + 0.05 * g * g
            w_out[at] = (w - 0.02 * (mean * lax.rsqrt(var + 1e-8) + 0.1 * w)).astype(BF)
            m_out[at] = mean
            v_out[at] = var

        if gathered:
            whole = rest[0]
            for n in range(64 // CUT):
                digits = (n // 16, n // 4 % 4, n % 4)
                x, y, z = (digits[(d - m) % 3] for d in range(3))
                whole[n * 16 : n * 16 + 16, :] = g_ref[x, y, z, 0, 0]
            look = lambda rows: whole[rows, :]
        else:
            look = lambda rows: g_ref[0, 0, rows, :]

        if m < 2:

            def one(b, c):
                rows = pl.ds(pl.multiple_of(b * 64, 64), 64)
                take((0, rows, slice(None)), look(rows))
                return c

            lax.fori_loop(0, D // CUT // 64, one, 0)
        else:

            def one(b, c):
                rows = pl.ds(pl.multiple_of(b * 128, 128), 128)
                take((0, slice(None), rows), look(rows).T)
                return c

            lax.fori_loop(0, D // CUT // 128, one, 0)


def adam(first, count, weights, means, variances, gradients, so_far=None):
    rows = D // CUT

    def place(j):
        s = first + j // CUT
        return jnp.where(s < NS, 1, 0), jnp.where(s < NS, s, s - NS), j % CUT

    def at_wide(j):
        layer, column, row = place(j)
        return layer, row, column

    wide = pl.BlockSpec((1, rows, SL), at_wide)
    tall = pl.BlockSpec((1, SL, rows), place)
    mine = [wide, wide, tall]
    gathered = so_far is not None
    if gathered:
        gradients = gradients.reshape(4, 4, 4, *gradients.shape[1:])

        def spec(m):
            return pl.BlockSpec(
                tuple(4 // CUT if d == m else 4 for d in range(3)) + (1, 1, 16, SL),
                lambda j: tuple(j % CUT if d == m else 0 for d in range(3)) + (m, j // CUT, 0, 0),
            )

    else:

        def spec(m):
            return pl.BlockSpec((1, 1, rows, SL), lambda j: (m, j // CUT, j % CUT, 0))

    shapes = [jax.ShapeDtypeStruct(a.shape, a.dtype) for a in (*weights, *means, *variances)]
    return pl.pallas_call(
        functools.partial(adam_kernel, gathered),
        name="adamw_rest" if gathered else "adamw",
        grid=(count * CUT,),
        in_specs=mine * 3 + [spec(m) for m in range(3)] + ([pl.BlockSpec(memory_space=pl.ANY)] * 9 if gathered else []),
        out_specs=mine * 3,
        out_shape=shapes,
        input_output_aliases={12 + k: k for k in range(9)} if gathered else {},
        scratch_shapes=[pltpu.VMEM((rows, SL), BF)] if gathered else [],
        compiler_params=pltpu.CompilerParams(vmem_limit_bytes=VMEM_LIMIT),
        cost_estimate=pl.CostEstimate(flops=10**10, bytes_accessed=66 * D * SL * count, transcendentals=3 * D * SL * count),
    )(*weights, *means, *variances, *[gradients] * 3, *(so_far or ()))


def solution(mesh):
    def step(x, dy, *arrays):
        x, dy = x[0], dy[0]
        weights, means, variances = (arrays[k : k + 3] for k in (0, 3, 6))
        g1, g0 = gradients(x, dy, *weights)
        g0 = lax.all_gather(g0, "dp", axis=0)
        new = adam(0, NS + Q, weights, means, variances, g1)
        return tuple(adam(NS + Q, NS - Q, weights, means, variances, g0, new))

    return jax.shard_map(
        step,
        mesh=mesh,
        in_specs=(P(("rep", "dp"), None, None),) * 2 + (P(None, None, None),) * 9,
        out_specs=(P("rep", None, None),) * 9,
        check_vma=False,
    )
```
